32 devices in a mesh: replica: 1 (over z), dp: 32 (over y, x, core).
Axes of the slice: x: 4, y: 4, z: 1, core: 2. Of those that a mesh axis runs over, the one named last changes fastest.
The devices are a block of a 4x4x8 slice.
Arguments:
- x: bfloat16 [1024, 256], P(('replica', 'dp'))
- lengths: int32 [1024], P(('replica', 'dp'))
- cache: bfloat16 [2, 1024, 512, 576], P(None, ('replica', 'dp'))
- w_q: bfloat16 [2, 256, 1152], replicated
- w_o: bfloat16 [2, 1024, 256], replicated
- expert_ids: int32 [2, 1024, 6], P(None, ('replica', 'dp'))
- slots: int32 [2, 1024, 6], P(None, ('replica', 'dp'))
- route_w: float32 [2, 1024, 6], P(None, ('replica', 'dp'))
- w1_exp: bfloat16 [2, 64, 256, 176], P(None, 'dp')
- w3_exp: bfloat16 [2, 64, 256, 176], P(None, 'dp')
- w2_exp: bfloat16 [2, 64, 176, 256], P(None, 'dp')
- w1_sh: bfloat16 [2, 256, 352], P(None, None, 'dp')
- w3_sh: bfloat16 [2, 256, 352], P(None, None, 'dp')
- w2_sh: bfloat16 [2, 352, 256], P(None, 'dp')
Outputs:
- output: bfloat16 [1024, 256], P(('replica', 'dp'))
All inputs are finite; a program needn't handle non-finite values.
Results may differ from the reference program's by a relative error of at most 0.02.
Values are sent between devices in bfloat16 or wider.
A program may use at most 768 MiB of HBM per device.

```python
import jax
import jax.numpy as jnp
from jax import lax

GROUP_SIZE = 32
BATCH_DEV = 32
SEQ_LEN = 512
D_MODEL = 256
NUM_HEADS = 2
EXPERTS = 64
TOP_K = 6
FF_EXPERT = 176
FF_SHARED = 352
CAPACITY = 6
LAYERS = 2
LATENT = 512
ROPE_DIM = 64

KV_DIM = LATENT + ROPE_DIM
TOKENS = GROUP_SIZE * BATCH_DEV
BUFFER_ROWS = EXPERTS * GROUP_SIZE * CAPACITY
ATT_SCALE = 1.0 / (192.0 ** 0.5)
NORM_EPS = 1e-6


def scaled_normal(key, shape, scale):
    return (jax.random.normal(key, shape, jnp.float32) * scale).astype(jnp.bfloat16)


def draw_routing(key):
    key_bias, key_score, key_hot = jax.random.split(key, 3)
    expert_bias = jax.random.randint(key_bias, (LAYERS, 1, EXPERTS), 0, 512)
    raw_score = jax.random.randint(key_score, (LAYERS, TOKENS, EXPERTS), 0, 1024) + expert_bias
    hot_expert = jax.random.randint(key_hot, (LAYERS, GROUP_SIZE, 1, 1), 0, EXPERTS)
    first_rows = jnp.arange(BATCH_DEV)[None, None, :, None] < CAPACITY
    forced = jnp.logical_and(first_rows, jnp.arange(EXPERTS)[None, None, None, :] == hot_expert)
    raw_score = raw_score + 4096 * forced.astype(jnp.int32).reshape(LAYERS, TOKENS, EXPERTS)
    ranked = raw_score * EXPERTS + jnp.arange(EXPERTS)
    expert_ids = lax.top_k(ranked, TOP_K)[1].astype(jnp.int32)
    member = (expert_ids[:, :, :, None] == jnp.arange(EXPERTS)).astype(jnp.int32)
    member = member.reshape(LAYERS, GROUP_SIZE, BATCH_DEV * TOP_K, EXPERTS)
    slot_rank = jnp.sum(jnp.cumsum(member, axis=2) * member, axis=-1) - 1
    slot_rank = slot_rank.reshape(LAYERS, TOKENS, TOP_K)
    slots = jnp.where(slot_rank < CAPACITY, slot_rank, -1).astype(jnp.int32)
    return expert_ids, slots


def setup_inputs(seed: int = 0, part: int = 0) -> dict:
    part_keys = jax.random.split(jax.random.fold_in(jax.random.key(seed), part), 5)
    weight_keys = jax.random.split(jax.random.key(seed + 1), 8)
    x = scaled_normal(part_keys[0], (TOKENS, D_MODEL), 1.0)
    lengths = jax.random.randint(part_keys[1], (TOKENS,), 1, SEQ_LEN + 1).at[0].set(SEQ_LEN).astype(jnp.int32)
    cache = scaled_normal(part_keys[2], (LAYERS, TOKENS, SEQ_LEN, KV_DIM), 1.0)
    expert_ids, slots = draw_routing(part_keys[3])
    route_w = jax.random.uniform(part_keys[4], (LAYERS, TOKENS, TOP_K), jnp.float32, 0.5, 1.5) * (3.0 / TOP_K)
    return dict(
        x=x,
        lengths=lengths,
        cache=cache,
        w_q=scaled_normal(weight_keys[0], (LAYERS, D_MODEL, NUM_HEADS * KV_DIM), 1.5 * D_MODEL ** -0.5),
        w_o=scaled_normal(weight_keys[1], (LAYERS, NUM_HEADS * LATENT, D_MODEL), (NUM_HEADS * LATENT) ** -0.5),
        expert_ids=expert_ids,
        slots=slots,
        route_w=route_w,
        w1_exp=scaled_normal(weight_keys[2], (LAYERS, EXPERTS, D_MODEL, FF_EXPERT), D_MODEL ** -0.5),
        w3_exp=scaled_normal(weight_keys[3], (LAYERS, EXPERTS, D_MODEL, FF_EXPERT), D_MODEL ** -0.5),
        w2_exp=scaled_normal(weight_keys[4], (LAYERS, EXPERTS, FF_EXPERT, D_MODEL), 1.5 * FF_EXPERT ** -0.5),
        w1_sh=scaled_normal(weight_keys[5], (LAYERS, D_MODEL, FF_SHARED), D_MODEL ** -0.5),
        w3_sh=scaled_normal(weight_keys[6], (LAYERS, D_MODEL, FF_SHARED), D_MODEL ** -0.5),
        w2_sh=scaled_normal(weight_keys[7], (LAYERS, FF_SHARED, D_MODEL), 2.0 * FF_SHARED ** -0.5),
    )


def rms_norm(values):
    vals32 = values.astype(jnp.float32)
    return vals32 * lax.rsqrt(jnp.mean(vals32 * vals32, axis=-1, keepdims=True) + NORM_EPS)


def attend_block(block_args):
    q_block, cache_block, len_block = block_args
    scores = jnp.einsum('bhc,btc->bht', q_block.astype(jnp.float32), cache_block.astype(jnp.float32)) * ATT_SCALE
    valid = jnp.arange(SEQ_LEN)[None, None, :] < len_block[:, None, None]
    probs = jax.nn.softmax(jnp.where(valid, scores, -jnp.inf), axis=-1)
    probs = probs.astype(jnp.bfloat16).astype(jnp.float32)
    return jnp.einsum('bht,btc->bhc', probs, cache_block[:, :, :LATENT].astype(jnp.float32))


def reference(x, lengths, cache, w_q, w_o, expert_ids, slots, route_w, w1_exp, w3_exp, w2_exp, w1_sh, w3_sh, w2_sh):
    owner_dev = jnp.arange(TOKENS) // BATCH_DEV
    len_blocks = lengths.reshape(GROUP_SIZE, BATCH_DEV)

    def layer_step(resid, layer_args):
        cache_l, w_q_l, w_o_l, ids_l, slot_l, gate_w, w1_e, w3_e, w2_e, w1_s, w3_s, w2_s = layer_args
        normed = rms_norm(resid).astype(jnp.bfloat16)
        queries = jnp.dot(normed, w_q_l, preferred_element_type=jnp.float32).astype(jnp.bfloat16)
        queries = queries.reshape(GROUP_SIZE, BATCH_DEV, NUM_HEADS, KV_DIM)
        attn = lax.map(attend_block, (queries, cache_l.reshape(GROUP_SIZE, BATCH_DEV, SEQ_LEN, KV_DIM), len_blocks))
        attn = attn.astype(jnp.bfloat16).reshape(TOKENS, NUM_HEADS * LATENT)
        resid = (resid.astype(jnp.float32) + jnp.dot(attn, w_o_l, preferred_element_type=jnp.float32)).astype(jnp.bfloat16)
        ffn_in = rms_norm(resid).astype(jnp.bfloat16)
        shared_gate = jnp.dot(ffn_in, w3_s, preferred_element_type=jnp.float32)
        shared_up = jnp.dot(ffn_in, w1_s, preferred_element_type=jnp.float32)
        shared_h = (jax.nn.silu(shared_gate) * shared_up).astype(jnp.bfloat16)
        shared_out = jnp.dot(shared_h, w2_s, preferred_element_type=jnp.float32)
        buf_rows = jnp.where(slot_l >= 0, ids_l * (GROUP_SIZE * CAPACITY) + owner_dev[:, None] * CAPACITY + slot_l, BUFFER_ROWS)
        copies = jnp.broadcast_to(ffn_in[:, None, :], (TOKENS, TOP_K, D_MODEL)).reshape(TOKENS * TOP_K, D_MODEL)
        buffer = jnp.zeros((BUFFER_ROWS, D_MODEL), jnp.bfloat16).at[buf_rows.reshape(-1)].set(copies, mode='drop')
        buffer = buffer.reshape(EXPERTS, GROUP_SIZE * CAPACITY, D_MODEL).astype(jnp.float32)
        gate_in = jnp.einsum('ecd,edf->ecf', buffer, w3_e.astype(jnp.float32))
        up_in = jnp.einsum('ecd,edf->ecf', buffer, w1_e.astype(jnp.float32))
        hidden = (jax.nn.silu(gate_in) * up_in).astype(jnp.bfloat16).astype(jnp.float32)
        expert_out = jnp.einsum('ecf,efd->ecd', hidden, w2_e.astype(jnp.float32)).astype(jnp.bfloat16)
        picked = jnp.take(expert_out.reshape(BUFFER_ROWS, D_MODEL), buf_rows, axis=0, mode='fill', fill_value=0)
        routed = jnp.sum(gate_w[:, :, None] * picked.astype(jnp.float32), axis=1)
        resid = (resid.astype(jnp.float32) + routed + shared_out).astype(jnp.bfloat16)
        return resid, None

    final_x = lax.scan(layer_step, x, (cache, w_q, w_o, expert_ids, slots, route_w, w1_exp, w3_exp, w2_exp, w1_sh, w3_sh, w2_sh))[0]
    return final_x
```

```python
import functools

import jax
import jax.numpy as jnp
from jax import lax
from jax.experimental import pallas as pl
from jax.experimental.pallas import tpu as pltpu
from jax.sharding import PartitionSpec as P

NORM_EPS = 1e-6
ATT_SCALE = 1.0 / (192.0 ** 0.5)
LATENT = 512
GROUP_SEQS = 8
SLOT_ROWS = 8
SHARD_ROWS = 16
F32 = jnp.float32
BF16 = jnp.bfloat16
MESH = pl.DeviceIdType.MESH
NT = (((1,), (1,)), ((), ()))


def rms_norm(vals32):
    return vals32 * lax.rsqrt(jnp.mean(vals32 * vals32, axis=-1, keepdims=True) + NORM_EPS)


def dot32(a, b):
    return jnp.dot(a, b, preferred_element_type=F32)


def dot_nt(a, b):
    return lax.dot_general(a, b, NT, preferred_element_type=F32)


def silu(v):
    return v * (1.0 / (1.0 + jnp.exp(-v)))


def step_kernel(
    group, lengths, x_ref, cache, w_q, w_o, ids_ref, slots_ref, rw_ref, w1e, w3e, w2e, w1s_ref, w3s_ref, w2s_ref,
    out_ref,
    cache_v, wq_v, wo_v, w1e_v, w3e_v, w2e_v, q_s, o_s, x_s, x1_s, ys_s,
    row_s, rwp_s, rwt_s, disp_s, sel_s, sh_send, sh_all, d_send, d_recv, r_send, r_recv,
    cache_sem, w_sem, sh_ssem, sh_rsem, d_ssem, d_rsem, r_ssem, r_rsem,
):
    me = lax.axis_index('dp')
    layers, batch = cache.shape[0], cache.shape[1]
    kv_dim = cache.shape[2]
    top_k = ids_ref.shape[0]
    local_experts = w1e.shape[1]
    shift = local_experts.bit_length() - 1
    d_model = x_ref.shape[1]
    n_rows = local_experts * group * SLOT_ROWS
    seq_len = cache.shape[3]

    def peer(i):
        return lax.rem(me + i, group)

    barrier = pltpu.get_barrier_semaphore()

    def greet(i, c):
        pl.semaphore_signal(barrier, inc=1, device_id={'dp': peer(i)}, device_id_type=MESH)
        return c

    lax.fori_loop(1, group, greet, 0)

    weight_copies = [
        pltpu.make_async_copy(src, dst, w_sem.at[i])
        for i, (src, dst) in enumerate(((w_q, wq_v), (w_o, wo_v), (w1e, w1e_v), (w3e, w3e_v), (w2e, w2e_v)))
    ]

    def cache_copy(l, b):
        return pltpu.make_async_copy(cache.at[l, b], cache_v.at[l, b], cache_sem.at[l, b])

    def start_cache(b, c):
        cache_copy(0, b).start()
        return c

    weight_copies[0].start()
    lax.fori_loop(0, batch, start_cache, 0)
    for cp in weight_copies[1:]:
        cp.start()

    for l in range(layers):
        for i, ref in enumerate((w1s_ref, w3s_ref, w2s_ref)):
            shard = ref[...].astype(F32)[:, l, :]
            sh_send[l, i] = jnp.zeros((SHARD_ROWS, d_model), BF16)
            sh_send[l, i, 0:shard.shape[0], :] = shard.astype(BF16)
            sh_all[l, i, me] = sh_send[l, i]
        ids = ids_ref[:, l, :]
        slots = slots_ref[:, l, :]
        rows = jnp.bitwise_and(ids, local_experts - 1) * (group * SLOT_ROWS) + jnp.right_shift(ids, shift) * SLOT_ROWS + slots
        rows = jnp.where(slots >= 0, rows, -1)
        r_iota = lax.broadcasted_iota(jnp.int32, (n_rows, batch), 0)
        disp = jnp.zeros((n_rows, batch), F32)
        for j in range(top_k):
            disp = jnp.where(r_iota == rows[j:j + 1, :], 1.0, disp)
        disp_s[l] = disp.astype(BF16)
        row_s[...] = jnp.full(row_s.shape, -1.0, F32)
        row_s[0:top_k, 0:batch] = rows.astype(F32)
        rwp_s[...] = jnp.zeros(rwp_s.shape, F32)
        rwp_s[0:top_k, 0:batch] = rw_ref[:, l, :]
        rows_t = row_s[...].T[0:batch, :]
        rwt_s[l] = rwp_s[...].T[0:batch, :]
        c_iota = lax.broadcasted_iota(jnp.int32, (batch, n_rows), 1).astype(F32)
        for j in range(top_k):
            sel_s[l, j * batch:(j + 1) * batch, :] = jnp.where(c_iota == rows_t[:, j:j + 1], 1.0, 0.0).astype(BF16)

    x_s[...] = x_ref[...].astype(F32)
    pl.semaphore_wait(barrier, group - 1)
    weight_copies[0].wait()

    row8 = jnp.bitwise_and(lax.broadcasted_iota(jnp.int32, (2 * GROUP_SEQS, seq_len), 0), GROUP_SEQS - 1)
    t_iota = lax.broadcasted_iota(jnp.int32, (2 * GROUP_SEQS, seq_len), 1)

    def sh_copy(l, i):
        return pltpu.make_async_remote_copy(
            src_ref=sh_send.at[l], dst_ref=sh_all.at[l, :, me], send_sem=sh_ssem.at[i], recv_sem=sh_rsem.at[i],
            device_id={'dp': peer(i)}, device_id_type=MESH)

    def d_copy(l, i):
        return pltpu.make_async_remote_copy(
            src_ref=d_send.at[l, :, peer(i)], dst_ref=d_recv.at[l, :, me], send_sem=d_ssem.at[i], recv_sem=d_rsem.at[i],
            device_id={'dp': peer(i)}, device_id_type=MESH)

    def r_copy(l, i):
        return pltpu.make_async_remote_copy(
            src_ref=r_send.at[l, :, peer(i)], dst_ref=r_recv.at[l, :, me], send_sem=r_ssem.at[i], recv_sem=r_rsem.at[i],
            device_id={'dp': peer(i)}, device_id_type=MESH)

    def each_peer(fn):
        def one(i, c):
            fn(i)
            return c
        lax.fori_loop(1, group, one, 0)

    def layer(l, carry):
        each_peer(lambda i: sh_copy(l, i).start())
        x = x_s[...]
        hidden = rms_norm(x).astype(BF16)
        q = dot32(hidden, wq_v[l]).astype(BF16).astype(F32)
        for g in range(batch // GROUP_SEQS):
            for h in range(2):
                q_s[g, h * GROUP_SEQS:(h + 1) * GROUP_SEQS, :] = q[g * GROUP_SEQS:(g + 1) * GROUP_SEQS, h * kv_dim:(h + 1) * kv_dim]

        def attend(g, c):
            qg = q_s[g].astype(BF16)
            base = g * GROUP_SEQS

            @pl.when(l + 1 < layers)
            def _():
                for j in range(GROUP_SEQS):
                    cache_copy(l + 1, base + j).start()

            s = jnp.full((2 * GROUP_SEQS, seq_len), -jnp.inf, F32)
            for j in range(GROUP_SEQS):
                cache_copy(l, base + j).wait()
                sj = dot32(qg, cache_v[l, base + j]) * ATT_SCALE
                keep = jnp.logical_and(row8 == j, t_iota < lengths[base + j])
                s = jnp.where(keep, sj, s)
            m = jnp.max(s, axis=-1, keepdims=True)
            e = jnp.exp(s - m)
            p = e * (1.0 / jnp.sum(e, axis=-1, keepdims=True))
            acc = jnp.zeros((LATENT, 2 * GROUP_SEQS), F32)
            for j in range(GROUP_SEQS):
                pj = jnp.where(row8 == j, p, 0.0).astype(BF16)
                acc = acc + dot_nt(cache_v[l, base + j, 0:LATENT, :], pj)
            og = acc.T
            rows_g = pl.ds(pl.multiple_of(base, GROUP_SEQS), GROUP_SEQS)
            o_s[rows_g, 0:LATENT] = og[0:GROUP_SEQS]
            o_s[rows_g, LATENT:2 * LATENT] = og[GROUP_SEQS:2 * GROUP_SEQS]
            return c

        lax.fori_loop(0, batch // GROUP_SEQS, attend, 0)

        @pl.when(l == 0)
        def _():
            for cp in weight_copies[1:]:
                cp.wait()

        x1 = (x + dot32(o_s[...].astype(BF16), wo_v[l])).astype(BF16).astype(F32)
        x1_s[...] = x1
        ffn_in = rms_norm(x1).astype(BF16)
        d_send[l] = dot32(disp_s[l], ffn_in).astype(BF16).reshape(local_experts, group, SLOT_ROWS, d_model)
        each_peer(lambda i: d_copy(l, i).start())
        d_recv[l, :, me] = d_send[l, :, me]

        each_peer(lambda i: sh_copy(l, i).wait_recv())
        hid = group * SHARD_ROWS
        up = dot_nt(ffn_in, sh_all[l, 0].reshape(hid, d_model))
        gate = dot_nt(ffn_in, sh_all[l, 1].reshape(hid, d_model))
        sh_h = (silu(gate) * up).astype(BF16)
        ys_s[...] = dot32(sh_h, sh_all[l, 2].reshape(hid, d_model))
        each_peer(lambda i: sh_copy(l, i).wait_send())

        each_peer(lambda i: d_copy(l, i).wait_recv())
        for n in range(local_experts):
            rows_in = d_recv[l, n].reshape(group * SLOT_ROWS, d_model)
            gate = dot_nt(rows_in, w3e_v[l, n])
            up = dot_nt(rows_in, w1e_v[l, n])
            eh = (silu(gate) * up).astype(BF16)
            r_send[l, n] = dot32(eh, w2e_v[l, n]).astype(BF16).reshape(group, SLOT_ROWS, d_model)
        each_peer(lambda i: r_copy(l, i).start())
        r_recv[l, :, me] = r_send[l, :, me]
        each_peer(lambda i: d_copy(l, i).wait_send())
        each_peer(lambda i: r_copy(l, i).wait_recv())
        picked = dot32(sel_s[l], r_recv[l].reshape(n_rows, d_model))
        rw = rwt_s[l]
        routed = rw[:, 0:1] * picked[0:batch]
        for j in range(1, top_k):
            routed = routed + rw[:, j:j + 1] * picked[j * batch:(j + 1) * batch]
        x_s[...] = (x1_s[...] + routed + ys_s[...]).astype(BF16).astype(F32)
        each_peer(lambda i: r_copy(l, i).wait_send())
        return carry

    lax.fori_loop(0, layers, layer, 0)
    out_ref[...] = x_s[...].astype(BF16)


def solution(mesh):
    group = mesh.shape['dp']
    tok_axes = ('replica', 'dp')
    in_specs = (
        P(tok_axes, None), P(tok_axes), P(None, tok_axes, None, None),
        P(None, None, None), P(None, None, None),
        P(None, tok_axes, None), P(None, tok_axes, None), P(None, tok_axes, None),
        P(None, 'dp', None, None), P(None, 'dp', None, None), P(None, 'dp', None, None),
        P(None, None, 'dp'), P(None, None, 'dp'), P(None, 'dp', None),
    )

    def device_step(x, lengths, cache, w_q, w_o, expert_ids, slots, route_w, w1_exp, w3_exp, w2_exp, w1_sh, w3_sh, w2_sh):
        batch, d_model = x.shape
        layers, _, seq_len, kv_dim = cache.shape
        local_experts, ff = w1_exp.shape[1], w1_exp.shape[3]
        top_k = expert_ids.shape[2]
        n_rows = local_experts * group * SLOT_ROWS
        vmem = pl.BlockSpec(memory_space=pltpu.VMEM)
        smem = pl.BlockSpec(memory_space=pltpu.SMEM)
        hbm = pl.BlockSpec(memory_space=pl.ANY)
        block = (layers, local_experts, group, SLOT_ROWS, d_model)
        scratch = [
            pltpu.VMEM((layers, batch, kv_dim, seq_len), BF16),
            pltpu.VMEM(w_q.shape, BF16),
            pltpu.VMEM(w_o.shape, BF16),
            pltpu.VMEM((layers, local_experts, ff, d_model), BF16),
            pltpu.VMEM((layers, local_experts, ff, d_model), BF16),
            pltpu.VMEM((layers, local_experts, ff, d_model), BF16),
            pltpu.VMEM((batch // GROUP_SEQS, 2 * GROUP_SEQS, kv_dim), F32),
            pltpu.VMEM((batch, 2 * LATENT), F32),
            pltpu.VMEM((batch, d_model), F32),
            pltpu.VMEM((batch, d_model), F32),
            pltpu.VMEM((batch, d_model), F32),
            pltpu.VMEM((8, 128), F32),
            pltpu.VMEM((8, 128), F32),
            pltpu.VMEM((layers, batch, 8), F32),
            pltpu.VMEM((layers, n_rows, batch), BF16),
            pltpu.VMEM((layers, top_k * batch, n_rows), BF16),
            pltpu.VMEM((layers, 3, SHARD_ROWS, d_model), BF16),
            pltpu.VMEM((layers, 3, group, SHARD_ROWS, d_model), BF16),
            pltpu.VMEM(block, BF16),
            pltpu.VMEM(block, BF16),
            pltpu.VMEM(block, BF16),
            pltpu.VMEM(block, BF16),
            pltpu.SemaphoreType.DMA((layers, batch)),
            pltpu.SemaphoreType.DMA((5,)),
        ] + [pltpu.SemaphoreType.DMA((group,))] * 6
        return pl.pallas_call(
            functools.partial(step_kernel, group),
            out_shape=jax.ShapeDtypeStruct((batch, d_model), BF16),
            in_specs=[smem, vmem, hbm, hbm, hbm, vmem, vmem, vmem, hbm, hbm, hbm, vmem, vmem, vmem],
            out_specs=vmem,
            scratch_shapes=scratch,
            compiler_params=pltpu.CompilerParams(collective_id=0, has_side_effects=True, vmem_limit_bytes=62 * 1024 * 1024),
        )(
            lengths, x, jnp.swapaxes(cache, 2, 3), w_q, w_o,
            jnp.transpose(expert_ids, (2, 0, 1)), jnp.transpose(slots, (2, 0, 1)), jnp.transpose(route_w, (2, 0, 1)),
            jnp.swapaxes(w1_exp, 2, 3), jnp.swapaxes(w3_exp, 2, 3), w2_exp,
            jnp.transpose(w1_sh, (2, 0, 1)), jnp.transpose(w3_sh, (2, 0, 1)), jnp.transpose(w2_sh, (1, 0, 2)),
        )

    return jax.shard_map(device_step, mesh=mesh, in_specs=in_specs, out_specs=P(tok_axes, None), check_vma=False)
```

```python
import functools

import jax
import jax.numpy as jnp
from jax import lax
from jax.experimental import pallas as pl
from jax.experimental.pallas import tpu as pltpu
from jax.sharding import PartitionSpec as P

NORM_EPS = 1e-6
ATT_SCALE = 1.0 / (192.0 ** 0.5)
LATENT = 512
GROUP_SEQS = 8
SLOT_ROWS = 8
SHARD_ROWS = 16
F32 = jnp.float32
BF16 = jnp.bfloat16
MESH = pl.DeviceIdType.MESH
NT = (((1,), (1,)), ((), ()))


def rms_norm(vals32):
    return vals32 * lax.rsqrt(jnp.mean(vals32 * vals32, axis=-1, keepdims=True) + NORM_EPS)


def dot32(a, b):
    return jnp.dot(a, b, preferred_element_type=F32)


def dot_nt(a, b):
    return lax.dot_general(a, b, NT, preferred_element_type=F32)


def silu(v):
    return v * (1.0 / (1.0 + jnp.exp(-v)))


def step_kernel(
    group, side, lengths, x_in, cache, w_q, w_o, ids_in, slots_in, rw_in, w1e, w3e, w2e, w1s, w3s, w2s,
    out_ref,
    len_s, x_v, ids_v, slots_v, rw_v, shard_v, cache_v, wq_v, wo_v, w1e_v, w3e_v, w2e_v, q_s, p_s, o_s, x_s, x1_s,
    row_s, rwp_s, rwt_s, disp_s, sel_s, sh_send, sh_all, d_send, d_recv, r_send, r_recv,
    cache_sem, in_sem, sh_ssem, sh_rsem, d_ssem, d_rsem, r_ssem, r_rsem,
):
    me = lax.axis_index('dp')
    core = lax.rem(me, 2)
    chip_x = lax.rem(me // 2, side)
    chip_y = me // (2 * side)
    layers, batch, kv_dim, seq_len = cache.shape
    top_k = ids_in.shape[0]
    local_experts = w1e.shape[1]
    shift = local_experts.bit_length() - 1
    d_model = x_in.shape[1]
    n_rows = local_experts * group * SLOT_ROWS
    n_groups = batch // GROUP_SEQS
    used = pl.ds(0, max(1, 2 * batch * top_k // (local_experts * group)))

    def at_offset(dy, dx, dc):
        return (lax.rem(chip_y + dy, side) * side + lax.rem(chip_x + dx, side)) * 2 + lax.rem(core + dc, 2)

    def far(offset):
        return -(min(offset[0], side - offset[0]) + min(offset[1], side - offset[1])), -offset[2]

    offsets = [(dy, dx, dc) for dy in range(side) for dx in range(side) for dc in range(2)]
    offsets = sorted(offsets, key=far)[:-1]
    assert side == 4

    row_a = chip_y + core * (chip_x - chip_y)
    col_b = chip_x + core * (chip_y - chip_x)

    def device_at(a, b):
        return ((a + core * (b - a)) * side + (b + core * (a - b))) * 2 + core

    copies = {
        name: pltpu.make_async_copy(src, dst, in_sem.at[i])
        for i, (name, src, dst) in enumerate((
            ('x', x_in, x_v), ('wq0', w_q.at[0], wq_v.at[0]), ('len', lengths, len_s),
            ('s0', w1s, shard_v.at[0]), ('s1', w3s, shard_v.at[1]), ('s2', w2s, shard_v.at[2]),
            ('ids', ids_in, ids_v), ('slots', slots_in, slots_v), ('rw', rw_in, rw_v),
            ('wo', w_o, wo_v), ('w1e', w1e, w1e_v), ('w3e', w3e, w3e_v), ('w2e', w2e, w2e_v),
            ('wq1', w_q.at[1:], wq_v.at[1:]),
        ))
    }

    def start_group(l, g):
        for j in range(GROUP_SEQS):
            b = g * GROUP_SEQS + j
            pltpu.make_async_copy(cache.at[l, b], cache_v.at[l, b], cache_sem.at[l, g]).start()

    def wait_group(l, g):
        rows = pl.ds(g * GROUP_SEQS, GROUP_SEQS)
        pltpu.make_async_copy(cache.at[l, rows], cache_v.at[l, rows], cache_sem.at[l, g]).wait()

    def start_layer(l, first=0):
        def one(g, c):
            start_group(l, g)
            return c
        lax.fori_loop(first, n_groups, one, 0)

    for name in ('x', 'wq0', 'len'):
        copies[name].start()
    start_group(0, 0)
    for name in ('s0', 's1', 's2', 'ids', 'slots'):
        copies[name].start()
    r_recv[...] = jnp.zeros(r_recv.shape, BF16)

    barrier = pltpu.get_barrier_semaphore()

    def greet(i, c):
        pl.semaphore_signal(barrier, inc=1, device_id={'dp': lax.rem(me + i, group)}, device_id_type=MESH)
        return c

    lax.fori_loop(1, group, greet, 0)
    start_layer(0, 1)
    for name in ('rw', 'wo', 'w1e', 'w3e', 'w2e', 'wq1'):
        copies[name].start()

    for i in range(3):
        copies[f's{i}'].wait()
    for i in range(3):
        shards = shard_v[i].astype(F32)
        for l in range(layers):
            sh_send[l, i] = jnp.zeros((SHARD_ROWS, d_model), BF16)
            sh_send[l, i, 0:shards.shape[0], :] = shards[:, l, :].astype(BF16)
    copies['ids'].wait()
    copies['slots'].wait()

    def routed_rows(l):
        ids = ids_v[:, l, :]
        slots = slots_v[:, l, :]
        rows = jnp.bitwise_and(ids, local_experts - 1) * (group * SLOT_ROWS) + jnp.right_shift(ids, shift) * SLOT_ROWS + slots
        return jnp.where(slots >= 0, rows, -1)

    def build_dispatch(l):
        rows = routed_rows(l)
        r_iota = lax.broadcasted_iota(jnp.int32, (n_rows, batch), 0)
        disp = jnp.zeros((n_rows, batch), F32)
        for j in range(top_k):
            disp = jnp.where(r_iota == rows[j:j + 1, :], 1.0, disp)
        disp_s[l] = disp.astype(BF16)

    def build_select(l):
        row_s[...] = jnp.full(row_s.shape, -1.0, F32)
        row_s[0:top_k, 0:batch] = routed_rows(l).astype(F32)
        rwp_s[...] = jnp.zeros(rwp_s.shape, F32)
        rwp_s[0:top_k, 0:batch] = rw_v[:, l, :]
        rows_t = row_s[...].T[0:batch, :]
        rwt_s[l] = rwp_s[...].T[0:batch, :]
        c_iota = lax.broadcasted_iota(jnp.int32, (batch, n_rows), 1).astype(F32)
        for j in range(top_k):
            sel_s[l, j * batch:(j + 1) * batch, :] = jnp.where(c_iota == rows_t[:, j:j + 1], 1.0, 0.0).astype(BF16)

    build_dispatch(0)
    copies['x'].wait()
    copies['wq0'].wait()
    copies['len'].wait()
    x_s[...] = x_v[...].astype(F32)

    row8 = jnp.bitwise_and(lax.broadcasted_iota(jnp.int32, (2 * GROUP_SEQS, seq_len), 0), GROUP_SEQS - 1)
    row8v = jnp.bitwise_and(lax.broadcasted_iota(jnp.int32, (2 * GROUP_SEQS, LATENT), 0), GROUP_SEQS - 1)
    t_iota = lax.broadcasted_iota(jnp.int32, (2 * GROUP_SEQS, seq_len), 1)

    def remote(src, dst, ssem, rsem, dev):
        return pltpu.make_async_remote_copy(
            src_ref=src, dst_ref=dst, send_sem=ssem, recv_sem=rsem, device_id={'dp': dev}, device_id_type=MESH)

    def wait_block(ref, sem):
        pltpu.make_async_copy(ref, ref, sem).wait()

    def wait_all_peers(ref, sem):
        wait_block(ref.at[:, pl.ds(0, group - 1), used], sem)

    def spread_1(l):
        sh_all[l, core, row_a, col_b] = sh_send[l]
        for k in (2, 1, 3):
            dev = device_at(row_a, lax.rem(col_b + k, side))
            remote(sh_send.at[l], sh_all.at[l, core, row_a, col_b], sh_ssem.at[0], sh_rsem.at[0], dev).start()

    def spread_2(l):
        wait_block(sh_all.at[l, 0, 0, pl.ds(0, side - 1)], sh_rsem.at[0])
        line = sh_all.at[l, core, row_a]
        for k in (1, side - 1):
            dev = device_at(lax.rem(row_a + k, side), col_b)
            remote(line, line, sh_ssem.at[1], sh_rsem.at[1], dev).start()

    def spread_3(l):
        wait_block(sh_all.at[l, 0, pl.ds(0, 2)], sh_rsem.at[1])
        for k, half in ((1, 0), (side - 1, side // 2)):
            dev = device_at(lax.rem(row_a + k, side), col_b)
            part = sh_all.at[l, core, lax.rem(row_a + side - k, side), pl.ds(half, side // 2)]
            remote(part, part, sh_ssem.at[2], sh_rsem.at[2], dev).start()

    def spread_4(l):
        wait_block(sh_all.at[l, 0, 0], sh_rsem.at[2])
        half = sh_all.at[l, core]
        remote(half, half, sh_ssem.at[3], sh_rsem.at[3], me + 1 - 2 * core).start()

    def spread_end(l):
        wait_block(sh_all.at[l, 0], sh_rsem.at[3])
        wait_block(sh_all.at[l, 0, 0, pl.ds(0, side - 1)], sh_ssem.at[0])
        wait_block(sh_all.at[l, 0, pl.ds(0, 2)], sh_ssem.at[1])
        wait_block(sh_all.at[l, 0, 0], sh_ssem.at[2])
        wait_block(sh_all.at[l, 0], sh_ssem.at[3])

    def layer(l, carry):
        x = x_s[...]
        hidden = rms_norm(x).astype(BF16)
        q = dot32(hidden, wq_v[l]).astype(BF16).astype(F32)
        for g in range(n_groups):
            for h in range(2):
                q_s[g, h * GROUP_SEQS:(h + 1) * GROUP_SEQS, :] = q[g * GROUP_SEQS:(g + 1) * GROUP_SEQS, h * kv_dim:(h + 1) * kv_dim]

        def score_step(s, qg, g, j):
            sj = dot32(qg, cache_v[l, g * GROUP_SEQS + j]) * ATT_SCALE
            keep = jnp.logical_and(row8 == j, t_iota < len_s[g * GROUP_SEQS + j])
            return jnp.where(keep, sj, s)

        def softmax(s):
            e = jnp.exp(s - jnp.max(s, axis=-1, keepdims=True))
            return e * (1.0 / jnp.sum(e, axis=-1, keepdims=True))

        def value_step(acc, p, g, j):
            return jnp.where(row8v == j, dot_nt(p, cache_v[l, g * GROUP_SEQS + j, 0:LATENT, :]), acc)

        def put_out(acc, g):
            og = acc
            rows_g = pl.ds(pl.multiple_of(g * GROUP_SEQS, GROUP_SEQS), GROUP_SEQS)
            o_s[rows_g, 0:LATENT] = og[0:GROUP_SEQS]
            o_s[rows_g, LATENT:2 * LATENT] = og[GROUP_SEQS:2 * GROUP_SEQS]

        no_score = jnp.full((2 * GROUP_SEQS, seq_len), -jnp.inf, F32)
        no_out = jnp.zeros((2 * GROUP_SEQS, LATENT), F32)

        wait_group(l, 0)
        s = no_score
        qg = q_s[0].astype(BF16)
        for j in range(GROUP_SEQS):
            s = score_step(s, qg, 0, j)
        p_s[...] = softmax(s)

        @pl.when(l == 0)
        def _():
            pl.semaphore_wait(barrier, group - 1)

        spread_1(l)

        def attend(g, c):
            wait_group(l, g + 1)
            p = p_s[...].astype(BF16)
            qg = q_s[g + 1].astype(BF16)
            s, acc = no_score, no_out
            for j in range(GROUP_SEQS):
                s = score_step(s, qg, g + 1, j)
                acc = value_step(acc, p, g, j)
            p_s[...] = softmax(s)
            put_out(acc, g)
            @pl.when(g == n_groups // 2 - 1)
            def _():
                spread_2(l)
            return c

        lax.fori_loop(0, n_groups - 1, attend, 0)
        p = p_s[...].astype(BF16)
        acc = no_out
        for j in range(GROUP_SEQS):
            acc = value_step(acc, p, n_groups - 1, j)
        put_out(acc, n_groups - 1)

        @pl.when(l == 0)
        def _():
            for name in ('wo', 'w1e', 'w3e', 'w2e', 'wq1', 'rw'):
                copies[name].wait()

        x1 = (x_s[...] + dot32(o_s[...].astype(BF16), wo_v[l])).astype(BF16).astype(F32)
        x1_s[...] = x1
        ffn_in = rms_norm(x1).astype(BF16)
        d_send[l] = dot32(disp_s[l], ffn_in).astype(BF16).reshape(local_experts, group, SLOT_ROWS, d_model)
        for off in offsets:
            dev = at_offset(*off)
            remote(d_send.at[l, :, dev, used], d_recv.at[l, :, me, used], d_ssem.at[0], d_rsem.at[0], dev).start()
        d_recv[l, :, me] = d_send[l, :, me]
        spread_3(l)

        @pl.when(l + 1 < layers)
        def _():
            start_layer(l + 1)

        @pl.when(l == 0)
        def _():
            for other in range(1, layers):
                build_dispatch(other)
            for other in range(layers):
                build_select(other)

        wait_all_peers(d_recv.at[l], d_rsem.at[0])
        spread_4(l)
        for n in range(local_experts):
            rows_in = d_recv[l, n].reshape(group * SLOT_ROWS, d_model)
            gate = dot_nt(rows_in, w3e_v[l, n])
            up = dot_nt(rows_in, w1e_v[l, n])
            eh = (silu(gate) * up).astype(BF16)
            r_send[l, n] = dot32(eh, w2e_v[l, n]).astype(BF16).reshape(group, SLOT_ROWS, d_model)
        for off in offsets:
            dev = at_offset(*off)
            remote(r_send.at[l, :, dev, used], r_recv.at[l, :, me, used], r_ssem.at[0], r_rsem.at[0], dev).start()
        r_recv[l, :, me] = r_send[l, :, me]
        spread_end(l)
        hid = group * SHARD_ROWS
        ffn_in = rms_norm(x1_s[...]).astype(BF16)
        up = dot_nt(ffn_in, sh_all[l, :, :, :, 0].reshape(hid, d_model))
        gate = dot_nt(ffn_in, sh_all[l, :, :, :, 1].reshape(hid, d_model))
        sh_h = (silu(gate) * up).astype(BF16)
        x1_s[...] = x1_s[...] + dot32(sh_h, sh_all[l, :, :, :, 2].reshape(hid, d_model))
        wait_all_peers(d_send.at[l], d_ssem.at[0])
        wait_all_peers(r_recv.at[l], r_rsem.at[0])
        picked = dot32(sel_s[l], r_recv[l].reshape(n_rows, d_model))
        rw = rwt_s[l]
        routed = rw[:, 0:1] * picked[0:batch]
        for j in range(1, top_k):
            routed = routed + rw[:, j:j + 1] * picked[j * batch:(j + 1) * batch]
        x_s[...] = (x1_s[...] + routed).astype(BF16).astype(F32)
        wait_all_peers(r_send.at[l], r_ssem.at[0])
        return carry

    lax.fori_loop(0, layers, layer, 0)
    out_ref[...] = x_s[...].astype(BF16)


def solution(mesh):
    group = mesh.shape['dp']
    side = 1
    while 2 * side * side < group:
        side += 1
    tok_axes = ('replica', 'dp')
    in_specs = (
        P(tok_axes, None), P(tok_axes), P(None, tok_axes, None, None),
        P(None, None, None), P(None, None, None),
        P(None, tok_axes, None), P(None, tok_axes, None), P(None, tok_axes, None),
        P(None, 'dp', None, None), P(None, 'dp', None, None), P(None, 'dp', None, None),
        P(None, None, 'dp'), P(None, None, 'dp'), P(None, 'dp', None),
    )

    def device_step(x, lengths, cache, w_q, w_o, expert_ids, slots, route_w, w1_exp, w3_exp, w2_exp, w1_sh, w3_sh, w2_sh):
        batch, d_model = x.shape
        layers, _, seq_len, kv_dim = cache.shape
        local_experts, ff = w1_exp.shape[1], w1_exp.shape[3]
        top_k = expert_ids.shape[2]
        n_rows = local_experts * group * SLOT_ROWS
        vmem = pl.BlockSpec(memory_space=pltpu.VMEM)
        hbm = pl.BlockSpec(memory_space=pl.ANY)
        block = (layers, local_experts, group, SLOT_ROWS, d_model)
        expert = (layers, local_experts, ff, d_model)
        route = (top_k, layers, batch)
        one_sem = pltpu.SemaphoreType.DMA((1,))
        scratch = [
            pltpu.SMEM((batch,), jnp.int32),
            pltpu.VMEM((batch, d_model), BF16),
            pltpu.VMEM(route, jnp.int32),
            pltpu.VMEM(route, jnp.int32),
            pltpu.VMEM(route, F32),
            pltpu.VMEM((3, w1_sh.shape[2], layers, d_model), BF16),
            pltpu.VMEM((layers, batch, kv_dim, seq_len), BF16),
            pltpu.VMEM(w_q.shape, BF16),
            pltpu.VMEM(w_o.shape, BF16),
            pltpu.VMEM(expert, BF16),
            pltpu.VMEM(expert, BF16),
            pltpu.VMEM(expert, BF16),
            pltpu.VMEM((batch // GROUP_SEQS, 2 * GROUP_SEQS, kv_dim), F32),
            pltpu.VMEM((2 * GROUP_SEQS, seq_len), F32),
            pltpu.VMEM((batch, 2 * LATENT), F32),
            pltpu.VMEM((batch, d_model), F32),
            pltpu.VMEM((batch, d_model), F32),
            pltpu.VMEM((8, 128), F32),
            pltpu.VMEM((8, 128), F32),
            pltpu.VMEM((layers, batch, 8), F32),
            pltpu.VMEM((layers, n_rows, batch), BF16),
            pltpu.VMEM((layers, top_k * batch, n_rows), BF16),
            pltpu.VMEM((layers, 3, SHARD_ROWS, d_model), BF16),
            pltpu.VMEM((layers, 2, side, side, 3, SHARD_ROWS, d_model), BF16),
            pltpu.VMEM(block, BF16),
            pltpu.VMEM(block, BF16),
            pltpu.VMEM(block, BF16),
            pltpu.VMEM(block, BF16),
            pltpu.SemaphoreType.DMA((layers, batch // GROUP_SEQS)),
            pltpu.SemaphoreType.DMA((14,)),
            pltpu.SemaphoreType.DMA((4,)),
            pltpu.SemaphoreType.DMA((4,)),
            one_sem, one_sem, one_sem, one_sem,
        ]
        return pl.pallas_call(
            functools.partial(step_kernel, group, side),
            out_shape=jax.ShapeDtypeStruct((batch, d_model), BF16),
            in_specs=[hbm] * 14,
            out_specs=vmem,
            scratch_shapes=scratch,
            compiler_params=pltpu.CompilerParams(collective_id=0, has_side_effects=True, vmem_limit_bytes=60 * 1024 * 1024),
        )(
            lengths, x, jnp.swapaxes(cache, 2, 3), w_q, w_o,
            jnp.transpose(expert_ids, (2, 0, 1)), jnp.transpose(slots, (2, 0, 1)), jnp.transpose(route_w, (2, 0, 1)),
            jnp.swapaxes(w1_exp, 2, 3), jnp.swapaxes(w3_exp, 2, 3), w2_exp,
            jnp.transpose(w1_sh, (2, 0, 1)), jnp.transpose(w3_sh, (2, 0, 1)), jnp.transpose(w2_sh, (1, 0, 2)),
        )

    return jax.shard_map(device_step, mesh=mesh, in_specs=in_specs, out_specs=P(tok_axes, None), check_vma=False)
```

```python
import functools

import jax
import jax.numpy as jnp
from jax import lax
from jax.experimental import pallas as pl
from jax.experimental.pallas import tpu as pltpu
from jax.sharding import PartitionSpec as P

NORM_EPS = 1e-6
ATT_SCALE = 1.0 / (192.0 ** 0.5)
LATENT = 512
GROUP_SEQS = 8
HALF = 4
TURNED = 5
SLOT_ROWS = 8
SHARD_ROWS = 16
F32 = jnp.float32
BF16 = jnp.bfloat16
MESH = pl.DeviceIdType.MESH
NT = (((1,), (1,)), ((), ()))


def rms_norm(vals32):
    return vals32 * lax.rsqrt(jnp.mean(vals32 * vals32, axis=-1, keepdims=True) + NORM_EPS)


def dot32(a, b):
    return jnp.dot(a, b, preferred_element_type=F32)


def dot_nt(a, b):
    return lax.dot_general(a, b, NT, preferred_element_type=F32)


def silu(v):
    return v * (1.0 / (1.0 + jnp.exp(-v)))


def step_kernel(
    group, side, lengths, x_in, cache, w_q, w_o, ids_in, slots_in, rw_in, w1e, w3e, w2e, w1s, w3s, w2s,
    out_ref,
    len_s, x_v, ids_v, slots_v, rw_v, shard_v, cache_v, wq_v, wo_v, w1e_v, w3e_v, w2e_v, q_s, p_s, o_s, x_s, x1_s,
    turn_s, row_s, rwp_s, rwt_s, disp_s, sel_s, sh_send, sh_all, d_send, d_recv, r_send, r_recv,
    cache_sem, in_sem, sh_ssem, sh_rsem, d_ssem, d_rsem, r_ssem, r_rsem,
):
    me = lax.axis_index('dp')
    core = lax.rem(me, 2)
    chip_x = lax.rem(me // 2, side)
    chip_y = me // (2 * side)
    layers, batch, kv_dim, seq_len = cache.shape
    top_k = ids_in.shape[0]
    local_experts = w1e.shape[1]
    shift = local_experts.bit_length() - 1
    d_model = x_in.shape[1]
    n_rows = local_experts * group * SLOT_ROWS
    n_groups = batch // GROUP_SEQS
    used = pl.ds(0, max(1, 2 * batch * top_k // (local_experts * group)))

    def at_offset(dy, dx, dc):
        return (lax.rem(chip_y + dy, side) * side + lax.rem(chip_x + dx, side)) * 2 + lax.rem(core + dc, 2)

    def far(offset):
        return -(min(offset[0], side - offset[0]) + min(offset[1], side - offset[1])), -offset[2]

    offsets = [(dy, dx, dc) for dy in range(side) for dx in range(side) for dc in range(2)]
    offsets = sorted(offsets, key=far)[:-1]
    assert side == 4 and layers == 2

    row_a = chip_y + core * (chip_x - chip_y)
    col_b = chip_x + core * (chip_y - chip_x)

    def device_at(a, b):
        return ((a + core * (b - a)) * side + (b + core * (a - b))) * 2 + core

    copies = {
        name: pltpu.make_async_copy(src, dst, in_sem.at[i])
        for i, (name, src, dst) in enumerate((
            ('x', x_in, x_v), ('wq0', w_q.at[0], wq_v.at[0]), ('len', lengths, len_s),
            ('s0', w1s, shard_v.at[0]), ('s1', w3s, shard_v.at[1]), ('s2', w2s, shard_v.at[2]),
            ('ids', ids_in, ids_v), ('slots', slots_in, slots_v), ('rw', rw_in, rw_v),
            ('wo', w_o, wo_v), ('w1e', w1e, w1e_v), ('w3e', w3e, w3e_v), ('w2e', w2e, w2e_v),
            ('wq1', w_q.at[1:], wq_v.at[1:]),
        ))
    }

    def start_half(l, k):
        def one(j, c):
            b = k * HALF + j
            pltpu.make_async_copy(cache.at[l, b], cache_v.at[l, b], cache_sem.at[l, k]).start()
            return c
        lax.fori_loop(0, HALF, one, 0, unroll=True)

    def start_halves(l, first, last):
        def one(k, c):
            start_half(l, k)
            return c
        lax.fori_loop(first, last, one, 0)

    def wait_half(l, k):
        rows = pl.ds(k * HALF, HALF)
        pltpu.make_async_copy(cache.at[l, rows], cache_v.at[l, rows], cache_sem.at[l, k]).wait()

    def wait_group(l, g):
        wait_half(l, 2 * g)
        wait_half(l, 2 * g + 1)

    n_halves = batch // HALF
    for name in ('x', 's0', 's1', 's2', 'ids', 'slots', 'len', 'wq0'):
        copies[name].start()
    start_half(0, 0)
    r_recv[...] = jnp.zeros(r_recv.shape, BF16)

    barrier = pltpu.get_barrier_semaphore()

    def greet(i, c):
        pl.semaphore_signal(barrier, inc=1, device_id={'dp': lax.rem(me + i, group)}, device_id_type=MESH)
        return c

    lax.fori_loop(1, group, greet, 0)
    start_halves(0, 1, n_halves)
    for name in ('rw', 'wo', 'w1e', 'w3e', 'w2e', 'wq1'):
        copies[name].start()

    for i in range(3):
        copies[f's{i}'].wait()
    for i in range(3):
        shards = shard_v[i].astype(F32)
        for l in range(layers):
            sh_send[l, i] = jnp.zeros((SHARD_ROWS, d_model), BF16)
            sh_send[l, i, 0:shards.shape[0], :] = shards[:, l, :].astype(BF16)
    copies['ids'].wait()
    copies['slots'].wait()

    def routed_rows(l):
        ids = ids_v[:, l, :]
        slots = slots_v[:, l, :]
        rows = jnp.bitwise_and(ids, local_experts - 1) * (group * SLOT_ROWS) + jnp.right_shift(ids, shift) * SLOT_ROWS + slots
        return jnp.where(slots >= 0, rows, -1)

    def build_dispatch(l):
        rows = routed_rows(l)
        r_iota = lax.broadcasted_iota(jnp.int32, (n_rows, batch), 0)
        disp = jnp.zeros((n_rows, batch), F32)
        for j in range(top_k):
            disp = jnp.where(r_iota == rows[j:j + 1, :], 1.0, disp)
        disp_s[l] = disp.astype(BF16)

    def build_select(l):
        row_s[...] = jnp.full(row_s.shape, -1.0, F32)
        row_s[0:top_k, 0:batch] = routed_rows(l).astype(F32)
        rwp_s[...] = jnp.zeros(rwp_s.shape, F32)
        rwp_s[0:top_k, 0:batch] = rw_v[:, l, :]
        rows_t = row_s[...].T[0:batch, :]
        rwt_s[l] = rwp_s[...].T[0:batch, :]
        c_iota = lax.broadcasted_iota(jnp.int32, (batch, n_rows), 1).astype(F32)
        for j in range(top_k):
            sel_s[l, j * batch:(j + 1) * batch, :] = jnp.where(c_iota == rows_t[:, j:j + 1], 1.0, 0.0).astype(BF16)

    build_dispatch(0)
    copies['x'].wait()
    copies['wq0'].wait()
    copies['len'].wait()
    x_s[...] = x_v[...].astype(F32)

    row8 = jnp.bitwise_and(lax.broadcasted_iota(jnp.int32, (2 * GROUP_SEQS, seq_len), 0), GROUP_SEQS - 1)
    row8v = jnp.bitwise_and(lax.broadcasted_iota(jnp.int32, (2 * GROUP_SEQS, LATENT), 0), GROUP_SEQS - 1)
    t_iota = lax.broadcasted_iota(jnp.int32, (2 * GROUP_SEQS, seq_len), 1)

    def remote(src, dst, ssem, rsem, dev):
        return pltpu.make_async_remote_copy(
            src_ref=src, dst_ref=dst, send_sem=ssem, recv_sem=rsem, device_id={'dp': dev}, device_id_type=MESH)

    def wait_block(ref, sem):
        pltpu.make_async_copy(ref, ref, sem).wait()

    def wait_all_peers(ref, sem):
        wait_block(ref.at[:, pl.ds(0, group - 1), used], sem)

    def spread_1(l):
        sh_all[l, core, row_a, col_b] = sh_send[l]
        for k in (2, 1, 3):
            dev = device_at(row_a, lax.rem(col_b + k, side))
            remote(sh_send.at[l], sh_all.at[l, core, row_a, col_b], sh_ssem.at[l, 0], sh_rsem.at[l, 0], dev).start()

    def spread_2(l):
        wait_block(sh_all.at[l, 0, 0, pl.ds(0, side - 1)], sh_rsem.at[l, 0])
        line = sh_all.at[l, core, row_a]
        for k in (1, side - 1):
            dev = device_at(lax.rem(row_a + k, side), col_b)
            remote(line, line, sh_ssem.at[l, 1], sh_rsem.at[l, 1], dev).start()

    def spread_3(l):
        wait_block(sh_all.at[l, 0, pl.ds(0, 2)], sh_rsem.at[l, 1])
        for k, half in ((1, 0), (side - 1, side // 2)):
            dev = device_at(lax.rem(row_a + k, side), col_b)
            part = sh_all.at[l, core, lax.rem(row_a + side - k, side), pl.ds(half, side // 2)]
            remote(part, part, sh_ssem.at[l, 2], sh_rsem.at[l, 2], dev).start()

    def spread_4(l):
        wait_block(sh_all.at[l, 0, 0], sh_rsem.at[l, 2])
        half = sh_all.at[l, core]
        remote(half, half, sh_ssem.at[l, 3], sh_rsem.at[l, 3], me + 1 - 2 * core).start()

    def spread_end(l):
        wait_block(sh_all.at[l, 0], sh_rsem.at[l, 3])
        wait_block(sh_all.at[l, 0, 0, pl.ds(0, side - 1)], sh_ssem.at[l, 0])
        wait_block(sh_all.at[l, 0, pl.ds(0, 2)], sh_ssem.at[l, 1])
        wait_block(sh_all.at[l, 0, 0], sh_ssem.at[l, 2])
        wait_block(sh_all.at[l, 0], sh_ssem.at[l, 3])

    def turn_ahead(l, first, last):
        if l + 1 >= layers:
            return

        def one(g, c):
            wait_group(l + 1, g)
            for j in range(GROUP_SEQS):
                b = g * GROUP_SEQS + j
                cache_v[0, b, 0:LATENT, :] = cache_v[l + 1, b, 0:LATENT, :].T
            return c

        lax.fori_loop(first, last, one, 0)

    for l in range(layers):
        if l > 0:
            spread_2(l)
        x = x_s[...]
        hidden = rms_norm(x).astype(BF16)
        q = dot32(hidden, wq_v[l]).astype(BF16).astype(F32)
        for g in range(n_groups):
            for h in range(2):
                q_s[g, h * GROUP_SEQS:(h + 1) * GROUP_SEQS, :] = q[g * GROUP_SEQS:(g + 1) * GROUP_SEQS, h * kv_dim:(h + 1) * kv_dim]

        def score_step(s, qg, g, j):
            sj = dot32(qg, cache_v[l, g * GROUP_SEQS + j]) * ATT_SCALE
            keep = jnp.logical_and(row8 == j, t_iota < len_s[g * GROUP_SEQS + j])
            return jnp.where(keep, sj, s)

        def softmax(s):
            e = jnp.exp(s - jnp.max(s, axis=-1, keepdims=True))
            return e * (1.0 / jnp.sum(e, axis=-1, keepdims=True))

        def value_step(acc, p, g, j):
            if l > 0:
                o = dot32(p, cache_v[0, g * GROUP_SEQS + j, 0:LATENT, :])
            elif j < TURNED:
                o = dot32(p, turn_s[g % 2 if isinstance(g, int) else lax.rem(g, 2), j])
            else:
                o = dot_nt(p, cache_v[l, g * GROUP_SEQS + j, 0:LATENT, :])
            return jnp.where(row8v == j, o, acc)

        def turn_step(g, j):
            if l == 0 and j < TURNED:
                slot = g % 2 if isinstance(g, int) else lax.rem(g, 2)
                turn_s[slot, j] = cache_v[l, g * GROUP_SEQS + j, 0:LATENT, :].T

        def put_out(acc, g):
            og = acc
            rows_g = pl.ds(pl.multiple_of(g * GROUP_SEQS, GROUP_SEQS), GROUP_SEQS)
            o_s[rows_g, 0:LATENT] = og[0:GROUP_SEQS]
            o_s[rows_g, LATENT:2 * LATENT] = og[GROUP_SEQS:2 * GROUP_SEQS]

        no_score = jnp.full((2 * GROUP_SEQS, seq_len), -jnp.inf, F32)
        no_out = jnp.zeros((2 * GROUP_SEQS, LATENT), F32)

        s = no_score
        qg = q_s[0].astype(BF16)
        for j in range(GROUP_SEQS):
            if l == 0 and j % HALF == 0:
                wait_half(l, j // HALF)
            s = score_step(s, qg, 0, j)
            turn_step(0, j)
        p_s[...] = softmax(s)

        if l == 0:
            pl.semaphore_wait(barrier, group - 1)
            spread_1(l)

        def attend(g, c):
            if l == 0:
                wait_group(l, g + 1)
            p = p_s[...].astype(BF16)
            qg = q_s[g + 1].astype(BF16)
            s, acc = no_score, no_out
            for j in range(GROUP_SEQS):
                s = score_step(s, qg, g + 1, j)
                acc = value_step(acc, p, g, j)
                turn_step(g + 1, j)
            p_s[...] = softmax(s)
            put_out(acc, g)
            @pl.when(g == n_groups // 2 - 1)
            def _():
                if l == 0:
                    spread_2(l)

            if l + 1 < layers:
                @pl.when(g == n_groups - 2)
                def _():
                    start_halves(l + 1, 0, n_halves)
            return c

        lax.fori_loop(0, n_groups - 1, attend, 0)
        p = p_s[...].astype(BF16)
        acc = no_out
        for j in range(GROUP_SEQS):
            acc = value_step(acc, p, n_groups - 1, j)
        put_out(acc, n_groups - 1)

        if l == 0:
            for name in ('wo', 'w1e', 'w3e', 'w2e', 'wq1', 'rw'):
                copies[name].wait()

        x1 = (x_s[...] + dot32(o_s[...].astype(BF16), wo_v[l])).astype(BF16).astype(F32)
        x1_s[...] = x1
        ffn_in = rms_norm(x1).astype(BF16)
        d_send[l] = dot32(disp_s[l], ffn_in).astype(BF16).reshape(local_experts, group, SLOT_ROWS, d_model)
        for off in offsets:
            dev = at_offset(*off)
            remote(d_send.at[l, :, dev, used], d_recv.at[l, :, me, used], d_ssem.at[0], d_rsem.at[0], dev).start()
        d_recv[l, :, me] = d_send[l, :, me]
        spread_3(l)
        build_select(l)
        if l + 1 < layers:
            build_dispatch(l + 1)
        turn_ahead(l, 0, n_groups // 2)
        wait_all_peers(d_recv.at[l], d_rsem.at[0])
        spread_4(l)
        for n in range(local_experts):
            rows_in = d_recv[l, n].reshape(group * SLOT_ROWS, d_model)
            gate = dot_nt(rows_in, w3e_v[l, n])
            up = dot_nt(rows_in, w1e_v[l, n])
            eh = (silu(gate) * up).astype(BF16)
            r_send[l, n] = dot32(eh, w2e_v[l, n]).astype(BF16).reshape(group, SLOT_ROWS, d_model)
        for off in offsets:
            dev = at_offset(*off)
            remote(r_send.at[l, :, dev, used], r_recv.at[l, :, me, used], r_ssem.at[0], r_rsem.at[0], dev).start()
        r_recv[l, :, me] = r_send[l, :, me]
        spread_end(l)
        if l + 1 < layers:
            spread_1(l + 1)
        hid = group * SHARD_ROWS
        ffn_in = rms_norm(x1_s[...]).astype(BF16)
        up = dot_nt(ffn_in, sh_all[l, :, :, :, 0].reshape(hid, d_model))
        gate = dot_nt(ffn_in, sh_all[l, :, :, :, 1].reshape(hid, d_model))
        sh_h = (silu(gate) * up).astype(BF16)
        x1_s[...] = x1_s[...] + dot32(sh_h, sh_all[l, :, :, :, 2].reshape(hid, d_model))
        wait_all_peers(d_send.at[l], d_ssem.at[0])
        turn_ahead(l, n_groups // 2, n_groups)
        wait_all_peers(r_recv.at[l], r_rsem.at[0])
        picked = dot32(sel_s[l], r_recv[l].reshape(n_rows, d_model))
        rw = rwt_s[l]
        routed = rw[:, 0:1] * picked[0:batch]
        for j in range(1, top_k):
            routed = routed + rw[:, j:j + 1] * picked[j * batch:(j + 1) * batch]
        x_s[...] = (x1_s[...] + routed).astype(BF16).astype(F32)
        wait_all_peers(r_send.at[l], r_ssem.at[0])
    out_ref[...] = x_s[...].astype(BF16)


def solution(mesh):
    group = mesh.shape['dp']
    side = 1
    while 2 * side * side < group:
        side += 1
    tok_axes = ('replica', 'dp')
    in_specs = (
        P(tok_axes, None), P(tok_axes), P(None, tok_axes, None, None),
        P(None, None, None), P(None, None, None),
        P(None, tok_axes, None), P(None, tok_axes, None), P(None, tok_axes, None),
        P(None, 'dp', None, None), P(None, 'dp', None, None), P(None, 'dp', None, None),
        P(None, None, 'dp'), P(None, None, 'dp'), P(None, 'dp', None),
    )

    def device_step(x, lengths, cache, w_q, w_o, expert_ids, slots, route_w, w1_exp, w3_exp, w2_exp, w1_sh, w3_sh, w2_sh):
        batch, d_model = x.shape
        layers, _, seq_len, kv_dim = cache.shape
        local_experts, ff = w1_exp.shape[1], w1_exp.shape[3]
        top_k = expert_ids.shape[2]
        n_rows = local_experts * group * SLOT_ROWS
        vmem = pl.BlockSpec(memory_space=pltpu.VMEM)
        hbm = pl.BlockSpec(memory_space=pltpu.HBM)
        block = (layers, local_experts, group, SLOT_ROWS, d_model)
        expert = (layers, local_experts, ff, d_model)
        route = (top_k, layers, batch)
        one_sem = pltpu.SemaphoreType.DMA((1,))
        scratch = [
            pltpu.SMEM((batch,), jnp.int32),
            pltpu.VMEM((batch, d_model), BF16),
            pltpu.VMEM(route, jnp.int32),
            pltpu.VMEM(route, jnp.int32),
            pltpu.VMEM(route, F32),
            pltpu.VMEM((3, w1_sh.shape[2], layers, d_model), BF16),
            pltpu.VMEM((layers, batch, kv_dim, seq_len), BF16),
            pltpu.VMEM(w_q.shape, BF16),
            pltpu.VMEM(w_o.shape, BF16),
            pltpu.VMEM(expert, BF16),
            pltpu.VMEM(expert, BF16),
            pltpu.VMEM(expert, BF16),
            pltpu.VMEM((batch // GROUP_SEQS, 2 * GROUP_SEQS, kv_dim), F32),
            pltpu.VMEM((2 * GROUP_SEQS, seq_len), F32),
            pltpu.VMEM((batch, 2 * LATENT), F32),
            pltpu.VMEM((batch, d_model), F32),
            pltpu.VMEM((batch, d_model), F32),
            pltpu.VMEM((2, TURNED, seq_len, LATENT), BF16),
            pltpu.VMEM((8, 128), F32),
            pltpu.VMEM((8, 128), F32),
            pltpu.VMEM((layers, batch, 8), F32),
            pltpu.VMEM((layers, n_rows, batch), BF16),
            pltpu.VMEM((layers, top_k * batch, n_rows), BF16),
            pltpu.VMEM((layers, 3, SHARD_ROWS, d_model), BF16),
            pltpu.VMEM((layers, 2, side, side, 3, SHARD_ROWS, d_model), BF16),
            pltpu.VMEM(block, BF16),
            pltpu.VMEM(block, BF16),
            pltpu.VMEM(block, BF16),
            pltpu.VMEM(block, BF16),
            pltpu.SemaphoreType.DMA((layers, batch // HALF)),
            pltpu.SemaphoreType.DMA((14,)),
            pltpu.SemaphoreType.DMA((layers, 4)),
            pltpu.SemaphoreType.DMA((layers, 4)),
            one_sem, one_sem, one_sem, one_sem,
        ]
        return pl.pallas_call(
            functools.partial(step_kernel, group, side),
            out_shape=pltpu.VMEM((batch, d_model), BF16),
            in_specs=[hbm] * 14,
            out_specs=vmem,
            scratch_shapes=scratch,
            compiler_params=pltpu.CompilerParams(collective_id=0, has_side_effects=True, vmem_limit_bytes=56 * 1024 * 1024),
        )(
            lengths, x, jnp.swapaxes(cache, 2, 3), w_q, w_o,
            jnp.transpose(expert_ids, (2, 0, 1)), jnp.transpose(slots, (2, 0, 1)), jnp.transpose(route_w, (2, 0, 1)),
            jnp.swapaxes(w1_exp, 2, 3), jnp.swapaxes(w3_exp, 2, 3), w2_exp,
            jnp.transpose(w1_sh, (2, 0, 1)), jnp.transpose(w3_sh, (2, 0, 1)), jnp.transpose(w2_sh, (1, 0, 2)),
        )

    return jax.shard_map(device_step, mesh=mesh, in_specs=in_specs, out_specs=P(tok_axes, None), check_vma=False)
```

```python
import functools

import jax
import jax.numpy as jnp
from jax import lax
from jax.experimental import pallas as pl
from jax.experimental.pallas import tpu as pltpu
from jax.sharding import PartitionSpec as P

NORM_EPS = 1e-6
ATT_SCALE = 1.0 / (192.0 ** 0.5)
LATENT = 512
GROUP_SEQS = 8
HALF = 4
TURNED = 7
TURNED_HALF = 4
SPREAD2_AT = 2
SLOT_ROWS = 8
SHARD_ROWS = 16
F32 = jnp.float32
BF16 = jnp.bfloat16
MESH = pl.DeviceIdType.MESH
NT = (((1,), (1,)), ((), ()))


def rms_norm(vals32):
    return vals32 * lax.rsqrt(jnp.mean(vals32 * vals32, axis=-1, keepdims=True) + NORM_EPS)


def dot32(a, b):
    return jnp.dot(a, b, preferred_element_type=F32)


def dot_nt(a, b):
    return lax.dot_general(a, b, NT, preferred_element_type=F32)


def silu(v):
    return v * (1.0 / (1.0 + jnp.exp(-v)))


def step_kernel(
    group, side, lengths, x_in, cache, w_q, w_o, ids_in, slots_in, rw_in, w1e, w3e, w2e, w1s, w3s, w2s,
    out_ref,
    len_s, x_v, ids_v, slots_v, rw_v, shard_v, cache_v, wq_v, wo_v, w1e_v, w3e_v, w2e_v, q_s, p_s, o_s, x_s, x1_s,
    turn_s, row_s, rwp_s, rwt_s, disp_s, sel_s, sh_send, sh_all, d_send, d_recv, r_send, r_recv,
    cache_sem, in_sem, sh_ssem, sh_rsem, d_ssem, d_rsem, r_ssem, r_rsem,
):
    me = lax.axis_index('dp')
    core = lax.rem(me, 2)
    chip_x = lax.rem(me // 2, side)
    chip_y = me // (2 * side)
    layers, batch, kv_dim, seq_len = cache.shape
    top_k = ids_in.shape[0]
    local_experts = w1e.shape[1]
    shift = local_experts.bit_length() - 1
    d_model = x_in.shape[1]
    n_rows = local_experts * group * SLOT_ROWS
    n_groups = batch // GROUP_SEQS
    used = pl.ds(0, max(1, 2 * batch * top_k // (local_experts * group)))

    def at_offset(dy, dx, dc):
        return (lax.rem(chip_y + dy, side) * side + lax.rem(chip_x + dx, side)) * 2 + lax.rem(core + dc, 2)

    def far(offset):
        return -(min(offset[0], side - offset[0]) + min(offset[1], side - offset[1])), -offset[2]

    offsets = [(dy, dx, dc) for dy in range(side) for dx in range(side) for dc in range(2)]
    offsets = sorted(offsets, key=far)[:-1]
    assert side == 4 and layers == 2

    row_a = chip_y + core * (chip_x - chip_y)
    col_b = chip_x + core * (chip_y - chip_x)

    def device_at(a, b):
        return ((a + core * (b - a)) * side + (b + core * (a - b))) * 2 + core

    copies = {
        name: pltpu.make_async_copy(src, dst, in_sem.at[i])
        for i, (name, src, dst) in enumerate((
            ('x', x_in, x_v), ('wq0', w_q.at[0], wq_v.at[0]), ('len', lengths, len_s),
            ('s0', w1s, shard_v.at[0]), ('s1', w3s, shard_v.at[1]), ('s2', w2s, shard_v.at[2]),
            ('ids', ids_in, ids_v), ('slots', slots_in, slots_v), ('rw', rw_in, rw_v),
            ('wo', w_o, wo_v), ('w1e', w1e, w1e_v), ('w3e', w3e, w3e_v), ('w2e', w2e, w2e_v),
            ('wq1', w_q.at[1:], wq_v.at[1:]),
        ))
    }

    def start_half(l, k):
        def one(j, c):
            b = k * HALF + j
            pltpu.make_async_copy(cache.at[l, b], cache_v.at[l, b], cache_sem.at[l, k]).start()
            return c
        lax.fori_loop(0, HALF, one, 0, unroll=True)

    def start_halves(l, first, last):
        def one(k, c):
            start_half(l, k)
            return c
        lax.fori_loop(first, last, one, 0)

    def wait_half(l, k):
        rows = pl.ds(k * HALF, HALF)
        pltpu.make_async_copy(cache.at[l, rows], cache_v.at[l, rows], cache_sem.at[l, k]).wait()

    def wait_group(l, g):
        wait_half(l, 2 * g)
        wait_half(l, 2 * g + 1)

    n_halves = batch // HALF
    for name in ('x', 's0', 's1', 's2', 'ids', 'slots', 'len', 'wq0'):
        copies[name].start()
    start_half(0, 0)
    r_recv[...] = jnp.zeros(r_recv.shape, BF16)

    barrier = pltpu.get_barrier_semaphore()

    def greet(i, c):
        pl.semaphore_signal(barrier, inc=1, device_id={'dp': lax.rem(me + i, group)}, device_id_type=MESH)
        return c

    lax.fori_loop(1, group, greet, 0)
    start_halves(0, 1, n_halves)
    for name in ('rw', 'wo', 'w1e', 'w3e', 'w2e', 'wq1'):
        copies[name].start()

    for i in range(3):
        copies[f's{i}'].wait()
    for i in range(3):
        shards = shard_v[i].astype(F32)
        for l in range(layers):
            sh_send[l, i] = jnp.zeros((SHARD_ROWS, d_model), BF16)
            sh_send[l, i, 0:shards.shape[0], :] = shards[:, l, :].astype(BF16)
    copies['ids'].wait()
    copies['slots'].wait()

    def routed_rows(l):
        ids = ids_v[:, l, :]
        slots = slots_v[:, l, :]
        rows = jnp.bitwise_and(ids, local_experts - 1) * (group * SLOT_ROWS) + jnp.right_shift(ids, shift) * SLOT_ROWS + slots
        return jnp.where(slots >= 0, rows, -1)

    def build_dispatch(l):
        rows = routed_rows(l)
        r_iota = lax.broadcasted_iota(jnp.int32, (n_rows, batch), 0)
        disp = jnp.zeros((n_rows, batch), F32)
        for j in range(top_k):
            disp = jnp.where(r_iota == rows[j:j + 1, :], 1.0, disp)
        disp_s[l] = disp.astype(BF16)

    def build_select(l):
        row_s[...] = jnp.full(row_s.shape, -1.0, F32)
        row_s[0:top_k, 0:batch] = routed_rows(l).astype(F32)
        rwp_s[...] = jnp.zeros(rwp_s.shape, F32)
        rwp_s[0:top_k, 0:batch] = rw_v[:, l, :]
        rows_t = row_s[...].T[0:batch, :]
        rwt_s[l] = rwp_s[...].T[0:batch, :]
        c_iota = lax.broadcasted_iota(jnp.int32, (batch, n_rows), 1).astype(F32)
        for j in range(top_k):
            sel_s[l, j * batch:(j + 1) * batch, :] = jnp.where(c_iota == rows_t[:, j:j + 1], 1.0, 0.0).astype(BF16)

    build_dispatch(0)
    copies['x'].wait()
    copies['wq0'].wait()
    copies['len'].wait()
    x_s[...] = x_v[...].astype(F32)

    row8 = jnp.bitwise_and(lax.broadcasted_iota(jnp.int32, (2 * GROUP_SEQS, seq_len), 0), GROUP_SEQS - 1)
    row8v = jnp.bitwise_and(lax.broadcasted_iota(jnp.int32, (2 * GROUP_SEQS, LATENT), 0), GROUP_SEQS - 1)
    t_iota = lax.broadcasted_iota(jnp.int32, (2 * GROUP_SEQS, seq_len), 1)

    def remote(src, dst, ssem, rsem, dev):
        return pltpu.make_async_remote_copy(
            src_ref=src, dst_ref=dst, send_sem=ssem, recv_sem=rsem, device_id={'dp': dev}, device_id_type=MESH)

    def wait_block(ref, sem):
        pltpu.make_async_copy(ref, ref, sem).wait()

    def wait_all_peers(ref, sem):
        wait_block(ref.at[:, pl.ds(0, group - 1), used], sem)

    def spread_1(l):
        sh_all[l, core, row_a, col_b] = sh_send[l]
        for k in (2, 1, 3):
            dev = device_at(row_a, lax.rem(col_b + k, side))
            remote(sh_send.at[l], sh_all.at[l, core, row_a, col_b], sh_ssem.at[l, 0], sh_rsem.at[l, 0], dev).start()

    def spread_2(l):
        wait_block(sh_all.at[l, 0, 0, pl.ds(0, side - 1)], sh_rsem.at[l, 0])
        line = sh_all.at[l, core, row_a]
        for k in (1, side - 1):
            dev = device_at(lax.rem(row_a + k, side), col_b)
            remote(line, line, sh_ssem.at[l, 1], sh_rsem.at[l, 1], dev).start()

    def spread_3(l):
        wait_block(sh_all.at[l, 0, pl.ds(0, 2)], sh_rsem.at[l, 1])
        for k, half in ((1, 0), (side - 1, side // 2)):
            dev = device_at(lax.rem(row_a + k, side), col_b)
            part = sh_all.at[l, core, lax.rem(row_a + side - k, side), pl.ds(half, side // 2)]
            remote(part, part, sh_ssem.at[l, 2], sh_rsem.at[l, 2], dev).start()

    def spread_4(l):
        wait_block(sh_all.at[l, 0, 0], sh_rsem.at[l, 2])
        half = sh_all.at[l, core]
        remote(half, half, sh_ssem.at[l, 3], sh_rsem.at[l, 3], me + 1 - 2 * core).start()

    def spread_end(l):
        wait_block(sh_all.at[l, 0], sh_rsem.at[l, 3])
        wait_block(sh_all.at[l, 0, 0, pl.ds(0, side - 1)], sh_ssem.at[l, 0])
        wait_block(sh_all.at[l, 0, pl.ds(0, 2)], sh_ssem.at[l, 1])
        wait_block(sh_all.at[l, 0, 0], sh_ssem.at[l, 2])
        wait_block(sh_all.at[l, 0], sh_ssem.at[l, 3])

    def turn_ahead(l, first, last):
        if l + 1 >= layers:
            return

        def one(g, c):
            wait_group(l + 1, g)
            for j in range(GROUP_SEQS):
                b = g * GROUP_SEQS + j
                cache_v[0, b, 0:LATENT, :] = cache_v[l + 1, b, 0:LATENT, :].T
            return c

        lax.fori_loop(first, last, one, 0)

    whole = [(b, GROUP_SEQS) for b in range(0, batch, GROUP_SEQS)]
    inner = [(b, GROUP_SEQS) for b in range(HALF, batch - HALF, GROUP_SEQS)]
    segments = [[(0, HALF)] + inner + [(batch - HALF, HALF)]] + [whole] * (layers - 1)

    for l in range(layers):
        if l > 0:
            spread_2(l)
        segs = segments[l]
        hidden = rms_norm(x_s[...]).astype(BF16)
        q = dot32(hidden, wq_v[l]).astype(BF16).astype(F32)
        for k, (start, count) in enumerate(segs):
            for b in range(start, start + count, HALF):
                for h in range(2):
                    row = h * GROUP_SEQS + b % GROUP_SEQS
                    q_s[k, row:row + HALF, :] = q[b:b + HALF, h * kv_dim:(h + 1) * kv_dim]

        def turned(k, b):
            return l == 0 and b - segs[k][0] < (TURNED if segs[k][1] == GROUP_SEQS else TURNED_HALF)

        def score_step(s, qg, k, b):
            sj = dot32(qg, cache_v[l, b]) * ATT_SCALE
            keep = jnp.logical_and(row8 == b % GROUP_SEQS, t_iota < len_s[b])
            if turned(k, b):
                turn_s[k % 2, b - segs[k][0]] = cache_v[l, b, 0:LATENT, :].T
            return jnp.where(keep, sj, s)

        def value_step(acc, p, k, b):
            if l > 0:
                o = dot32(p, cache_v[0, b, 0:LATENT, :])
            elif turned(k, b):
                o = dot32(p, turn_s[k % 2, b - segs[k][0]])
            else:
                o = dot_nt(p, cache_v[l, b, 0:LATENT, :])
            return jnp.where(row8v == b % GROUP_SEQS, o, acc)

        def softmax(s):
            e = jnp.exp(s - jnp.max(s, axis=-1, keepdims=True))
            return e * (1.0 / jnp.sum(e, axis=-1, keepdims=True))

        def attend(before, k):
            s, acc, p, qg = None, None, None, None
            steps = []
            if k is not None:
                if l == 0:
                    for b in range(segs[k][0], sum(segs[k]), HALF) if k < last else ():
                        wait_half(l, b // HALF)
                s, qg = jnp.full((2 * GROUP_SEQS, seq_len), -jnp.inf, F32), q_s[k].astype(BF16)
            if before is not None:
                acc, p = jnp.zeros((2 * GROUP_SEQS, LATENT), F32), p_s[...].astype(BF16)
            for j in range(GROUP_SEQS):
                if k is not None and j < segs[k][1]:
                    s = score_step(s, qg, k, segs[k][0] + j)
                if before is not None and j < segs[before][1]:
                    acc = value_step(acc, p, before, segs[before][0] + j)
            if k is not None:
                p_s[...] = softmax(s)
            if before is not None:
                for b in range(segs[before][0], sum(segs[before]), HALF):
                    for h in range(2):
                        row = h * GROUP_SEQS + b % GROUP_SEQS
                        o_s[b:b + HALF, h * LATENT:(h + 1) * LATENT] = acc[row:row + HALF]

        last = len(segs) - 1
        for k in range(len(segs) + 1):
            if l + 1 < layers and k == last:
                for b in range(segs[k][0], sum(segs[k]), HALF):
                    wait_half(l, b // HALF)
                start_halves(l + 1, 0, n_halves)
            attend(k - 1 if k > 0 else None, k if k <= last else None)
            if l == 0 and k == 0:
                pl.semaphore_wait(barrier, group - 1)
                spread_1(l)
            if l == 0 and k == SPREAD2_AT:
                spread_2(l)

        if l == 0:
            for name in ('wo', 'w1e', 'w3e', 'w2e', 'wq1', 'rw'):
                copies[name].wait()

        x1 = (x_s[...] + dot32(o_s[...].astype(BF16), wo_v[l])).astype(BF16).astype(F32)
        x1_s[...] = x1
        ffn_in = rms_norm(x1).astype(BF16)
        d_send[l] = dot32(disp_s[l], ffn_in).astype(BF16).reshape(local_experts, group, SLOT_ROWS, d_model)
        for off in offsets:
            dev = at_offset(*off)
            remote(d_send.at[l, :, dev, used], d_recv.at[l, :, me, used], d_ssem.at[0], d_rsem.at[0], dev).start()
        d_recv[l, :, me] = d_send[l, :, me]
        spread_3(l)
        build_select(l)
        if l + 1 < layers:
            build_dispatch(l + 1)
        turn_ahead(l, 0, n_groups // 2)
        wait_all_peers(d_recv.at[l], d_rsem.at[0])
        spread_4(l)
        for n in range(local_experts):
            rows_in = d_recv[l, n].reshape(group * SLOT_ROWS, d_model)
            gate = dot_nt(rows_in, w3e_v[l, n])
            up = dot_nt(rows_in, w1e_v[l, n])
            eh = (silu(gate) * up).astype(BF16)
            r_send[l, n] = dot32(eh, w2e_v[l, n]).astype(BF16).reshape(group, SLOT_ROWS, d_model)
        for off in offsets:
            dev = at_offset(*off)
            remote(r_send.at[l, :, dev, used], r_recv.at[l, :, me, used], r_ssem.at[0], r_rsem.at[0], dev).start()
        r_recv[l, :, me] = r_send[l, :, me]
        spread_end(l)
        if l + 1 < layers:
            spread_1(l + 1)
        hid = group * SHARD_ROWS
        ffn_in = rms_norm(x1_s[...]).astype(BF16)
        up = dot_nt(ffn_in, sh_all[l, :, :, :, 0].reshape(hid, d_model))
        gate = dot_nt(ffn_in, sh_all[l, :, :, :, 1].reshape(hid, d_model))
        sh_h = (silu(gate) * up).astype(BF16)
        x1_s[...] = x1_s[...] + dot32(sh_h, sh_all[l, :, :, :, 2].reshape(hid, d_model))
        wait_all_peers(d_send.at[l], d_ssem.at[0])
        turn_ahead(l, n_groups // 2, n_groups)
        wait_all_peers(r_recv.at[l], r_rsem.at[0])
        picked = dot32(sel_s[l], r_recv[l].reshape(n_rows, d_model))
        rw = rwt_s[l]
        routed = rw[:, 0:1] * picked[0:batch]
        for j in range(1, top_k):
            routed = routed + rw[:, j:j + 1] * picked[j * batch:(j + 1) * batch]
        x_s[...] = (x1_s[...] + routed).astype(BF16).astype(F32)
        wait_all_peers(r_send.at[l], r_ssem.at[0])
    out_ref[...] = x_s[...].astype(BF16)


def solution(mesh):
    group = mesh.shape['dp']
    side = 1
    while 2 * side * side < group:
        side += 1
    tok_axes = ('replica', 'dp')
    in_specs = (
        P(tok_axes, None), P(tok_axes), P(None, tok_axes, None, None),
        P(None, None, None), P(None, None, None),
        P(None, tok_axes, None), P(None, tok_axes, None), P(None, tok_axes, None),
        P(None, 'dp', None, None), P(None, 'dp', None, None), P(None, 'dp', None, None),
        P(None, None, 'dp'), P(None, None, 'dp'), P(None, 'dp', None),
    )

    def device_step(x, lengths, cache, w_q, w_o, expert_ids, slots, route_w, w1_exp, w3_exp, w2_exp, w1_sh, w3_sh, w2_sh):
        batch, d_model = x.shape
        layers, _, seq_len, kv_dim = cache.shape
        local_experts, ff = w1_exp.shape[1], w1_exp.shape[3]
        top_k = expert_ids.shape[2]
        n_rows = local_experts * group * SLOT_ROWS
        vmem = pl.BlockSpec(memory_space=pltpu.VMEM)
        hbm = pl.BlockSpec(memory_space=pltpu.HBM)
        block = (layers, local_experts, group, SLOT_ROWS, d_model)
        expert = (layers, local_experts, ff, d_model)
        route = (top_k, layers, batch)
        one_sem = pltpu.SemaphoreType.DMA((1,))
        scratch = [
            pltpu.SMEM((batch,), jnp.int32),
            pltpu.VMEM((batch, d_model), BF16),
            pltpu.VMEM(route, jnp.int32),
            pltpu.VMEM(route, jnp.int32),
            pltpu.VMEM(route, F32),
            pltpu.VMEM((3, w1_sh.shape[2], layers, d_model), BF16),
            pltpu.VMEM((layers, batch, kv_dim, seq_len), BF16),
            pltpu.VMEM(w_q.shape, BF16),
            pltpu.VMEM(w_o.shape, BF16),
            pltpu.VMEM(expert, BF16),
            pltpu.VMEM(expert, BF16),
            pltpu.VMEM(expert, BF16),
            pltpu.VMEM((batch // GROUP_SEQS + 1, 2 * GROUP_SEQS, kv_dim), F32),
            pltpu.VMEM((2 * GROUP_SEQS, seq_len), F32),
            pltpu.VMEM((batch, 2 * LATENT), F32),
            pltpu.VMEM((batch, d_model), F32),
            pltpu.VMEM((batch, d_model), F32),
            pltpu.VMEM((2, TURNED, seq_len, LATENT), BF16),
            pltpu.VMEM((8, 128), F32),
            pltpu.VMEM((8, 128), F32),
            pltpu.VMEM((layers, batch, 8), F32),
            pltpu.VMEM((layers, n_rows, batch), BF16),
            pltpu.VMEM((layers, top_k * batch, n_rows), BF16),
            pltpu.VMEM((layers, 3, SHARD_ROWS, d_model), BF16),
            pltpu.VMEM((layers, 2, side, side, 3, SHARD_ROWS, d_model), BF16),
            pltpu.VMEM(block, BF16),
            pltpu.VMEM(block, BF16),
            pltpu.VMEM(block, BF16),
            pltpu.VMEM(block, BF16),
            pltpu.SemaphoreType.DMA((layers, batch // HALF)),
            pltpu.SemaphoreType.DMA((14,)),
            pltpu.SemaphoreType.DMA((layers, 4)),
            pltpu.SemaphoreType.DMA((layers, 4)),
            one_sem, one_sem, one_sem, one_sem,
        ]
        return pl.pallas_call(
            functools.partial(step_kernel, group, side),
            out_shape=pltpu.VMEM((batch, d_model), BF16),
            in_specs=[hbm] * 14,
            out_specs=vmem,
            scratch_shapes=scratch,
            compiler_params=pltpu.CompilerParams(collective_id=0, has_side_effects=True, vmem_limit_bytes=56 * 1024 * 1024),
        )(
            lengths, x, jnp.swapaxes(cache, 2, 3), w_q, w_o,
            jnp.transpose(expert_ids, (2, 0, 1)), jnp.transpose(slots, (2, 0, 1)), jnp.transpose(route_w, (2, 0, 1)),
            jnp.swapaxes(w1_exp, 2, 3), jnp.swapaxes(w3_exp, 2, 3), w2_exp,
            jnp.transpose(w1_sh, (2, 0, 1)), jnp.transpose(w3_sh, (2, 0, 1)), jnp.transpose(w2_sh, (1, 0, 2)),
        )

    return jax.shard_map(device_step, mesh=mesh, in_specs=in_specs, out_specs=P(tok_axes, None), check_vma=False)
```

```python
import functools

import jax
import jax.numpy as jnp
from jax import lax
from jax.experimental import pallas as pl
from jax.experimental.pallas import tpu as pltpu
from jax.sharding import PartitionSpec as P

NORM_EPS = 1e-6
ATT_SCALE = 1.0 / (192.0 ** 0.5)
LATENT = 512
GROUP_SEQS = 8
HALF = 4
TURNED = 7
TURNED_HALF = 4
SPREAD2_AT = 2
SLOT_ROWS = 8
SHARD_ROWS = 16
F32 = jnp.float32
BF16 = jnp.bfloat16
MESH = pl.DeviceIdType.MESH
NT = (((1,), (1,)), ((), ()))


def rms_norm(vals32):
    return vals32 * lax.rsqrt(jnp.mean(vals32 * vals32, axis=-1, keepdims=True) + NORM_EPS)


def dot32(a, b):
    return jnp.dot(a, b, preferred_element_type=F32)


def dot_nt(a, b):
    return lax.dot_general(a, b, NT, preferred_element_type=F32)


def silu(v):
    return v * (1.0 / (1.0 + jnp.exp(-v)))


def step_kernel(
    group, side, lengths, x_in, cache, w_q, w_o, ids_in, slots_in, rw_in, w1e, w3e, w2e, w1s, w3s, w2s,
    out_ref,
    len_s, x_v, ids_v, slots_v, rw_v, shard_v, cache_v, wq_v, wo_v, w1e_v, w3e_v, w2e_v, q_s, p_s, o_s, x_s, x1_s,
    turn_s, row_s, rwp_s, rwt_s, disp_s, sel_s, sh_send, sh_all, d_send, d_recv, r_send, r_recv,
    cache_sem, in_sem, sh_ssem, sh_rsem, d_ssem, d_rsem, r_ssem, r_rsem,
):
    me = lax.axis_index('dp')
    core = lax.rem(me, 2)
    chip_x = lax.rem(me // 2, side)
    chip_y = me // (2 * side)
    layers, batch, kv_dim, seq_len = cache.shape
    top_k = ids_in.shape[0]
    local_experts = w1e.shape[1]
    shift = local_experts.bit_length() - 1
    d_model = x_in.shape[1]
    n_rows = local_experts * group * SLOT_ROWS
    n_groups = batch // GROUP_SEQS
    used = pl.ds(0, max(1, 2 * batch * top_k // (local_experts * group)))

    def at_offset(dy, dx, dc):
        return (lax.rem(chip_y + dy, side) * side + lax.rem(chip_x + dx, side)) * 2 + lax.rem(core + dc, 2)

    def far(offset):
        return -(min(offset[0], side - offset[0]) + min(offset[1], side - offset[1])), -offset[2]

    offsets = [(dy, dx, dc) for dy in range(side) for dx in range(side) for dc in range(2)]
    offsets = sorted(offsets, key=far)[:-1]
    assert side == 4 and layers == 2

    row_a = chip_y + core * (chip_x - chip_y)
    col_b = chip_x + core * (chip_y - chip_x)

    def device_at(a, b):
        return ((a + core * (b - a)) * side + (b + core * (a - b))) * 2 + core

    copies = {
        name: pltpu.make_async_copy(src, dst, in_sem.at[i])
        for i, (name, src, dst) in enumerate((
            ('x', x_in, x_v), ('wq0', w_q.at[0], wq_v.at[0]), ('len', lengths, len_s),
            ('s0', w1s, shard_v.at[0]), ('s1', w3s, shard_v.at[1]), ('s2', w2s, shard_v.at[2]),
            ('ids', ids_in, ids_v), ('slots', slots_in, slots_v), ('rw', rw_in, rw_v),
            ('wo', w_o, wo_v), ('w1e', w1e, w1e_v), ('w3e', w3e, w3e_v), ('w2e', w2e, w2e_v),
            ('wq1', w_q.at[1:], wq_v.at[1:]),
        ))
    }

    def cache_slot(l, k):
        return k if l == 0 else batch // HALF + k // 2

    def start_half(l, k):
        def one(j, c):
            b = k * HALF + j
            pltpu.make_async_copy(cache.at[l, b], cache_v.at[l, b], cache_sem.at[cache_slot(l, k)]).start()
            return c
        lax.fori_loop(0, HALF, one, 0, unroll=True)

    def start_halves(l, first, last):
        def one(k, c):
            start_half(l, k)
            return c
        lax.fori_loop(first, last, one, 0)

    def wait_half(l, k):
        rows = pl.ds(k * HALF, HALF)
        pltpu.make_async_copy(cache.at[l, rows], cache_v.at[l, rows], cache_sem.at[cache_slot(l, k)]).wait()

    def wait_group(l, g):
        rows = pl.ds(g * GROUP_SEQS, GROUP_SEQS)
        pltpu.make_async_copy(cache.at[l, rows], cache_v.at[l, rows], cache_sem.at[cache_slot(l, 2 * g)]).wait()

    n_halves = batch // HALF
    for name in ('x', 's0', 's1', 's2', 'ids', 'slots', 'len', 'wq0'):
        copies[name].start()
    start_half(0, 0)
    r_recv[...] = jnp.zeros(r_recv.shape, BF16)

    barrier = pltpu.get_barrier_semaphore()

    def greet(i, c):
        pl.semaphore_signal(barrier, inc=1, device_id={'dp': lax.rem(me + i, group)}, device_id_type=MESH)
        return c

    lax.fori_loop(1, group, greet, 0)
    start_halves(0, 1, n_halves)
    for name in ('rw', 'wo', 'w1e', 'w3e', 'w2e', 'wq1'):
        copies[name].start()

    for i in range(3):
        copies[f's{i}'].wait()
    for i in range(3):
        shards = shard_v[i].astype(F32)
        for l in range(layers):
            sh_send[l, i] = jnp.zeros((SHARD_ROWS, d_model), BF16)
            sh_send[l, i, 0:shards.shape[0], :] = shards[:, l, :].astype(BF16)
    copies['ids'].wait()
    copies['slots'].wait()

    def routed_rows(l):
        ids = ids_v[:, l, :]
        slots = slots_v[:, l, :]
        rows = jnp.bitwise_and(ids, local_experts - 1) * (group * SLOT_ROWS) + jnp.right_shift(ids, shift) * SLOT_ROWS + slots
        return jnp.where(slots >= 0, rows, -1)

    def build_dispatch(l):
        rows = routed_rows(l)
        r_iota = lax.broadcasted_iota(jnp.int32, (n_rows, batch), 0)
        disp = jnp.zeros((n_rows, batch), F32)
        for j in range(top_k):
            disp = jnp.where(r_iota == rows[j:j + 1, :], 1.0, disp)
        disp_s[l] = disp.astype(BF16)

    def build_select(l):
        row_s[...] = jnp.full(row_s.shape, -1.0, F32)
        row_s[0:top_k, 0:batch] = routed_rows(l).astype(F32)
        rwp_s[...] = jnp.zeros(rwp_s.shape, F32)
        rwp_s[0:top_k, 0:batch] = rw_v[:, l, :]
        rows_t = row_s[...].T[0:batch, :]
        rwt_s[l] = rwp_s[...].T[0:batch, :]
        c_iota = lax.broadcasted_iota(jnp.int32, (batch, n_rows), 1).astype(F32)
        for j in range(top_k):
            sel_s[l, j * batch:(j + 1) * batch, :] = jnp.where(c_iota == rows_t[:, j:j + 1], 1.0, 0.0).astype(BF16)

    build_dispatch(0)
    copies['x'].wait()
    copies['wq0'].wait()
    copies['len'].wait()
    x_s[...] = x_v[...].astype(F32)

    row8 = jnp.bitwise_and(lax.broadcasted_iota(jnp.int32, (2 * GROUP_SEQS, seq_len), 0), GROUP_SEQS - 1)
    row8v = jnp.bitwise_and(lax.broadcasted_iota(jnp.int32, (2 * GROUP_SEQS, LATENT), 0), GROUP_SEQS - 1)
    t_iota = lax.broadcasted_iota(jnp.int32, (2 * GROUP_SEQS, seq_len), 1)

    def remote(src, dst, ssem, rsem, dev):
        return pltpu.make_async_remote_copy(
            src_ref=src, dst_ref=dst, send_sem=ssem, recv_sem=rsem, device_id={'dp': dev}, device_id_type=MESH)

    def wait_block(ref, sem):
        pltpu.make_async_copy(ref, ref, sem).wait()

    def wait_all_peers(ref, sem):
        wait_block(ref.at[:, pl.ds(0, group - 1), used], sem)

    def spread_1(l):
        sh_all[l, core, row_a, col_b] = sh_send[l]
        for k in (2, 1, 3):
            dev = device_at(row_a, lax.rem(col_b + k, side))
            remote(sh_send.at[l], sh_all.at[l, core, row_a, col_b], sh_ssem.at[0], sh_rsem.at[0], dev).start()

    def spread_2(l):
        wait_block(sh_all.at[l, 0, 0, pl.ds(0, side - 1)], sh_rsem.at[0])
        line = sh_all.at[l, core, row_a]
        for k in (1, side - 1):
            dev = device_at(lax.rem(row_a + k, side), col_b)
            remote(line, line, sh_ssem.at[1], sh_rsem.at[1], dev).start()

    def spread_3(l):
        wait_block(sh_all.at[l, 0, pl.ds(0, 2)], sh_rsem.at[1])
        for k, half in ((1, 0), (side - 1, side // 2)):
            dev = device_at(lax.rem(row_a + k, side), col_b)
            part = sh_all.at[l, core, lax.rem(row_a + side - k, side), pl.ds(half, side // 2)]
            remote(part, part, sh_ssem.at[2], sh_rsem.at[2], dev).start()

    def spread_4(l):
        wait_block(sh_all.at[l, 0, 0], sh_rsem.at[2])
        half = sh_all.at[l, core]
        remote(half, half, sh_ssem.at[3], sh_rsem.at[3], me + 1 - 2 * core).start()

    def spread_end(l):
        wait_block(sh_all.at[l, 0], sh_rsem.at[3])
        wait_block(sh_all.at[l, 0, 0, pl.ds(0, side - 1)], sh_ssem.at[0])
        wait_block(sh_all.at[l, 0, pl.ds(0, 2)], sh_ssem.at[1])
        wait_block(sh_all.at[l, 0, 0], sh_ssem.at[2])
        wait_block(sh_all.at[l, 0], sh_ssem.at[3])

    def turn_ahead(l, first, last):
        if l + 1 >= layers:
            return

        def one(g, c):
            wait_group(l + 1, g)
            for j in range(GROUP_SEQS):
                b = g * GROUP_SEQS + j
                cache_v[0, b, 0:LATENT, :] = cache_v[l + 1, b, 0:LATENT, :].T
            return c

        lax.fori_loop(first, last, one, 0)

    whole = [(b, GROUP_SEQS) for b in range(0, batch, GROUP_SEQS)]
    inner = [(b, GROUP_SEQS) for b in range(HALF, batch - HALF, GROUP_SEQS)]
    segments = [[(0, HALF)] + inner + [(batch - HALF, HALF)]] + [whole] * (layers - 1)

    for l in range(layers):
        if l > 0:
            spread_2(l)
        segs = segments[l]
        hidden = rms_norm(x_s[...]).astype(BF16)
        q = dot32(hidden, wq_v[l]).astype(BF16).astype(F32)
        for k, (start, count) in enumerate(segs):
            for b in range(start, start + count, HALF):
                for h in range(2):
                    row = h * GROUP_SEQS + b % GROUP_SEQS
                    q_s[k, row:row + HALF, :] = q[b:b + HALF, h * kv_dim:(h + 1) * kv_dim]

        def turned(k, b):
            return l == 0 and b - segs[k][0] < (TURNED if segs[k][1] == GROUP_SEQS else TURNED_HALF)

        def score_step(s, qg, k, b):
            sj = dot32(qg, cache_v[l, b]) * ATT_SCALE
            keep = jnp.logical_and(row8 == b % GROUP_SEQS, t_iota < len_s[b])
            if turned(k, b):
                turn_s[k % 2, b - segs[k][0]] = cache_v[l, b, 0:LATENT, :].T
            return jnp.where(keep, sj, s)

        def value_step(acc, p, k, b):
            if l > 0:
                o = dot32(p, cache_v[0, b, 0:LATENT, :])
            elif turned(k, b):
                o = dot32(p, turn_s[k % 2, b - segs[k][0]])
            else:
                o = dot_nt(p, cache_v[l, b, 0:LATENT, :])
            return jnp.where(row8v == b % GROUP_SEQS, o, acc)

        def softmax(s):
            e = jnp.exp(s - jnp.max(s, axis=-1, keepdims=True))
            return e * (1.0 / jnp.sum(e, axis=-1, keepdims=True))

        def attend(before, k):
            s, acc, p, qg = None, None, None, None
            steps = []
            if k is not None:
                if l == 0:
                    for b in range(segs[k][0], sum(segs[k]), HALF) if k < last else ():
                        wait_half(l, b // HALF)
                s, qg = jnp.full((2 * GROUP_SEQS, seq_len), -jnp.inf, F32), q_s[k].astype(BF16)
            if before is not None:
                acc, p = jnp.zeros((2 * GROUP_SEQS, LATENT), F32), p_s[...].astype(BF16)
            for j in range(GROUP_SEQS):
                if k is not None and j < segs[k][1]:
                    s = score_step(s, qg, k, segs[k][0] + j)
                if before is not None and j < segs[before][1]:
                    acc = value_step(acc, p, before, segs[before][0] + j)
            if k is not None:
                p_s[...] = softmax(s)
            if before is not None:
                for b in range(segs[before][0], sum(segs[before]), HALF):
                    for h in range(2):
                        row = h * GROUP_SEQS + b % GROUP_SEQS
                        o_s[b:b + HALF, h * LATENT:(h + 1) * LATENT] = acc[row:row + HALF]

        last = len(segs) - 1
        for k in range(len(segs) + 1):
            if l + 1 < layers and k == last:
                for b in range(segs[k][0], sum(segs[k]), HALF):
                    wait_half(l, b // HALF)
                start_halves(l + 1, 0, n_halves)
            attend(k - 1 if k > 0 else None, k if k <= last else None)
            if l == 0 and k == 0:
                pl.semaphore_wait(barrier, group - 1)
                spread_1(l)
            if l == 0 and k == SPREAD2_AT:
                spread_2(l)

        if l == 0:
            for name in ('wo', 'w1e', 'w3e', 'w2e', 'wq1', 'rw'):
                copies[name].wait()

        x1 = (x_s[...] + dot32(o_s[...].astype(BF16), wo_v[l])).astype(BF16).astype(F32)
        x1_s[...] = x1
        ffn_in = rms_norm(x1).astype(BF16)
        d_send[l] = dot32(disp_s[l], ffn_in).astype(BF16).reshape(local_experts, group, SLOT_ROWS, d_model)
        for off in offsets:
            dev = at_offset(*off)
            remote(d_send.at[l, :, dev, used], d_recv.at[l, :, me, used], d_ssem.at[0], d_rsem.at[0], dev).start()
        d_recv[l, :, me] = d_send[l, :, me]
        spread_3(l)
        build_select(l)
        if l + 1 < layers:
            build_dispatch(l + 1)
        turn_ahead(l, 0, n_groups // 2)
        wait_all_peers(d_recv.at[l], d_rsem.at[0])
        spread_4(l)
        for n in range(local_experts):
            rows_in = d_recv[l, n].reshape(group * SLOT_ROWS, d_model)
            gate = dot_nt(rows_in, w3e_v[l, n])
            up = dot_nt(rows_in, w1e_v[l, n])
            eh = (silu(gate) * up).astype(BF16)
            r_send[l, n] = dot32(eh, w2e_v[l, n]).astype(BF16).reshape(group, SLOT_ROWS, d_model)
        for off in offsets:
            dev = at_offset(*off)
            remote(r_send.at[l, :, dev, used], r_recv.at[l, :, me, used], r_ssem.at[0], r_rsem.at[0], dev).start()
        r_recv[l, :, me] = r_send[l, :, me]
        spread_end(l)
        if l + 1 < layers:
            spread_1(l + 1)
        hid = group * SHARD_ROWS
        ffn_in = rms_norm(x1_s[...]).astype(BF16)
        up = dot_nt(ffn_in, sh_all[l, :, :, :, 0].reshape(hid, d_model))
        gate = dot_nt(ffn_in, sh_all[l, :, :, :, 1].reshape(hid, d_model))
        sh_h = (silu(gate) * up).astype(BF16)
        x1_s[...] = x1_s[...] + dot32(sh_h, sh_all[l, :, :, :, 2].reshape(hid, d_model))
        wait_all_peers(d_send.at[l], d_ssem.at[0])
        turn_ahead(l, n_groups // 2, n_groups)
        wait_all_peers(r_recv.at[l], r_rsem.at[0])
        picked = dot32(sel_s[l], r_recv[l].reshape(n_rows, d_model))
        rw = rwt_s[l]
        routed = rw[:, 0:1] * picked[0:batch]
        for j in range(1, top_k):
            routed = routed + rw[:, j:j + 1] * picked[j * batch:(j + 1) * batch]
        x_s[...] = (x1_s[...] + routed).astype(BF16).astype(F32)
        wait_all_peers(r_send.at[l], r_ssem.at[0])
    out_ref[...] = x_s[...].astype(BF16)


def solution(mesh):
    group = mesh.shape['dp']
    side = 1
    while 2 * side * side < group:
        side += 1
    tok_axes = ('replica', 'dp')
    in_specs = (
        P(tok_axes, None), P(tok_axes), P(None, tok_axes, None, None),
        P(None, None, None), P(None, None, None),
        P(None, tok_axes, None), P(None, tok_axes, None), P(None, tok_axes, None),
        P(None, 'dp', None, None), P(None, 'dp', None, None), P(None, 'dp', None, None),
        P(None, None, 'dp'), P(None, None, 'dp'), P(None, 'dp', None),
    )

    def device_step(x, lengths, cache, w_q, w_o, expert_ids, slots, route_w, w1_exp, w3_exp, w2_exp, w1_sh, w3_sh, w2_sh):
        batch, d_model = x.shape
        layers, _, seq_len, kv_dim = cache.shape
        local_experts, ff = w1_exp.shape[1], w1_exp.shape[3]
        top_k = expert_ids.shape[2]
        n_rows = local_experts * group * SLOT_ROWS
        vmem = pl.BlockSpec(memory_space=pltpu.VMEM)
        hbm = pl.BlockSpec(memory_space=pltpu.HBM)
        block = (layers, local_experts, group, SLOT_ROWS, d_model)
        expert = (layers, local_experts, ff, d_model)
        route = (top_k, layers, batch)
        one_sem = pltpu.SemaphoreType.DMA((1,))
        scratch = [
            pltpu.SMEM((batch,), jnp.int32),
            pltpu.VMEM((batch, d_model), BF16),
            pltpu.VMEM(route, jnp.int32),
            pltpu.VMEM(route, jnp.int32),
            pltpu.VMEM(route, F32),
            pltpu.VMEM((3, w1_sh.shape[2], layers, d_model), BF16),
            pltpu.VMEM((layers, batch, kv_dim, seq_len), BF16),
            pltpu.VMEM(w_q.shape, BF16),
            pltpu.VMEM(w_o.shape, BF16),
            pltpu.VMEM(expert, BF16),
            pltpu.VMEM(expert, BF16),
            pltpu.VMEM(expert, BF16),
            pltpu.VMEM((batch // GROUP_SEQS + 1, 2 * GROUP_SEQS, kv_dim), F32),
            pltpu.VMEM((2 * GROUP_SEQS, seq_len), F32),
            pltpu.VMEM((batch, 2 * LATENT), F32),
            pltpu.VMEM((batch, d_model), F32),
            pltpu.VMEM((batch, d_model), F32),
            pltpu.VMEM((2, TURNED, seq_len, LATENT), BF16),
            pltpu.VMEM((8, 128), F32),
            pltpu.VMEM((8, 128), F32),
            pltpu.VMEM((layers, batch, 8), F32),
            pltpu.VMEM((layers, n_rows, batch), BF16),
            pltpu.VMEM((layers, top_k * batch, n_rows), BF16),
            pltpu.VMEM((layers, 3, SHARD_ROWS, d_model), BF16),
            pltpu.VMEM((layers, 2, side, side, 3, SHARD_ROWS, d_model), BF16),
            pltpu.VMEM(block, BF16),
            pltpu.VMEM(block, BF16),
            pltpu.VMEM(block, BF16),
            pltpu.VMEM(block, BF16),
            pltpu.SemaphoreType.DMA((batch // HALF + batch // GROUP_SEQS,)),
            pltpu.SemaphoreType.DMA((14,)),
            pltpu.SemaphoreType.DMA((4,)),
            pltpu.SemaphoreType.DMA((4,)),
            one_sem, one_sem, one_sem, one_sem,
        ]
        return pl.pallas_call(
            functools.partial(step_kernel, group, side),
            out_shape=pltpu.VMEM((batch, d_model), BF16),
            in_specs=[hbm] * 14,
            out_specs=vmem,
            scratch_shapes=scratch,
            compiler_params=pltpu.CompilerParams(collective_id=0, has_side_effects=True, vmem_limit_bytes=56 * 1024 * 1024),
        )(
            lengths, x, jnp.swapaxes(cache, 2, 3), w_q, w_o,
            jnp.transpose(expert_ids, (2, 0, 1)), jnp.transpose(slots, (2, 0, 1)), jnp.transpose(route_w, (2, 0, 1)),
            jnp.swapaxes(w1_exp, 2, 3), jnp.swapaxes(w3_exp, 2, 3), w2_exp,
            jnp.transpose(w1_sh, (2, 0, 1)), jnp.transpose(w3_sh, (2, 0, 1)), jnp.transpose(w2_sh, (1, 0, 2)),
        )

    return jax.shard_map(device_step, mesh=mesh, in_specs=in_specs, out_specs=P(tok_axes, None), check_vma=False)
```
